32 devices in a mesh: gx: 4 (over y, x), gy: 4 (over z), gz: 2 (over core).
Axes of the slice: x: 2, y: 2, z: 4, core: 2. Of those that a mesh axis runs over, the one named last changes fastest.
Arguments:
- offsets: float32 [3, 4, 16, 16, 128], P(None, 'gx', 'gy', 'gz'), may hold values from 0 to 10
- history: float32 [6, 4, 16, 16, 128], P(None, 'gx', 'gy', 'gz'), may hold values from -0.6 to 0.6
- occupied: int32 [4, 16, 16, 128], P('gx', 'gy', 'gz'), may hold values from 0 to 1, as said below
- species: int32 [4, 16, 16, 128], P('gx', 'gy', 'gz'), may hold values from 0 to 3
- chi_table: float32 [4], replicated, may hold values from 3 to 8
- eta_table: float32 [4], replicated, may hold values from 6 to 16
- gamma_table: float32 [4], replicated, may hold values from 0.5 to 1
Outputs:
- charge: float32 [4, 16, 16, 128], P('gx', 'gy', 'gz')
- residual: float32 [4, 16, 16, 128], P('gx', 'gy', 'gz')
The draws below stay inside these ranges and needn't reach their ends.
Inputs may be any that keep to these rules, and one draw needn't show every extreme that they name: `occupied`: slot 0 of every cell holds an atom.
All inputs are finite; a program needn't handle non-finite values.
Results may differ from the reference program's by a relative error of at most 0.0003.
Values sent between devices are 32-bit elements; how exact they have to be, the bound alone decides.
No kernel may reach another device: no remote copies, remote signals or barrier semaphores. Data moves between devices by JAX's collectives and lax.ppermute only.
A program may use at most 64 MiB of HBM per device.

```python
import jax
import jax.numpy as jnp
from jax import lax

SLOTS = 128
HIST = 6
NTYPES = 4
NX = 4
NY = 16
NZ = 16


def draw_occupied(key, part):
    levels = jax.random.randint(key, (NX, NY, NZ, SLOTS), 0, 1000)
    column = jnp.arange(NX, dtype=jnp.int32)[:, None, None, None]
    barrier = 300 + 650 * column // max(NX - 1, 1)
    filled = (levels < barrier).astype(jnp.int32)
    first = (jnp.arange(SLOTS, dtype=jnp.int32) == 0)[None, None, None, :]
    return jnp.where(first, 1, filled).astype(jnp.int32)


def place_ends(entries, rng, least, high):
    index_at = [jax.random.randint(jax.random.fold_in(rng, axis), (), 0, length) for axis, length in enumerate(entries.shape)]
    longest = entries.shape.index(max(entries.shape))
    next_to = index_at[:longest] + [(index_at[longest] + 1) % entries.shape[longest]] + index_at[longest + 1:]
    return entries.at[tuple(index_at)].set(least).at[tuple(next_to)].set(high)


def shard_levels(own_key, shape, pieces, low, high):
    def one(position, parts):
        steps = jax.random.uniform(jax.random.fold_in(jax.random.fold_in(own_key, 6), position), (parts,), jnp.float32, low / len(pieces), high / len(pieces))
        return jnp.repeat(jnp.exp(steps), shape[position] // parts).reshape((-1,) + (1,) * (len(shape) - position - 1))

    level = one(*pieces[0])
    for cut in pieces[1:]:
        level = level * one(*cut)
    return level


def gaussian(rng, shape, width, reach, pieces=(), kind=jnp.bfloat16):
    factor_of = shard_levels(rng, shape, pieces, -0.22, 0.18) if pieces else 1.0
    array = jax.random.normal(rng, shape, jnp.float32) * width * factor_of
    return jnp.minimum(jnp.maximum(array, -reach), reach).astype(kind)


def setup_inputs(seed: int = 0) -> dict:
    arg_keys = jax.random.split(jax.random.key(seed), 8)
    offsets = jnp.clip(10.0 * jax.random.uniform(arg_keys[0], (3, NX, NY, NZ, SLOTS), jnp.float32) ** shard_levels(arg_keys[0], (3, NX, NY, NZ, SLOTS), ((1, 4), (2, 4), (3, 2)), -0.2, 0.2), 0.0, 10.0)
    history = gaussian(arg_keys[1], (HIST, NX, NY, NZ, SLOTS), 0.1, 0.6, ((1, 4), (2, 4), (3, 2)), jnp.float32)
    occupied = draw_occupied(jax.random.fold_in(arg_keys[7], 71), 0)
    species = place_ends(jax.random.randint(arg_keys[3], (NX, NY, NZ, SLOTS), 0, NTYPES), jax.random.fold_in(arg_keys[3], 1), 0, NTYPES - 1).astype(jnp.int32)
    chi_table = jnp.clip(jax.random.uniform(arg_keys[4], (NTYPES,), jnp.float32, 3.0, 8.0), 3.0, 8.0)
    eta_table = jnp.clip(jax.random.uniform(arg_keys[5], (NTYPES,), jnp.float32, 6.0, 16.0), 6.0, 16.0)
    gamma_table = jnp.clip(jax.random.uniform(arg_keys[6], (NTYPES,), jnp.float32, 0.5, 1.0), 0.5, 1.0)
    return dict(offsets=offsets, history=history, occupied=occupied, species=species, chi_table=chi_table, eta_table=eta_table, gamma_table=gamma_table)


EDGE = 10.0
CUTOFF = 10.0
COULOMB = 14.4
extrapolate_weights = (22.0 / 7.0, -55.0 / 14.0, 55.0 / 21.0, -22.0 / 21.0, 5.0 / 21.0, -1.0 / 42.0)

def lookup(species, values_table):
    match = species[..., None] == jnp.arange(values_table.shape[0], dtype=jnp.int32)
    return lax.optimization_barrier(jnp.sum(jnp.where(match, values_table, jnp.float32(0.0)), axis=-1))

def pair_sum(target, source, shifts):
    delta_x = source[0][..., None, :] + shifts[0] - target[0][..., :, None]
    delta_y = source[1][..., None, :] + shifts[1] - target[1][..., :, None]
    delta_z = source[2][..., None, :] + shifts[2] - target[2][..., :, None]
    square = delta_x * delta_x + delta_y * delta_y + delta_z * delta_z
    radius = jnp.sqrt(square)
    ratio = radius / CUTOFF
    fourth = ratio * ratio * ratio * ratio
    polynom = 1.0 + fourth * (-35.0 + ratio * (84.0 + ratio * (-70.0 + 20.0 * ratio)))
    tapered = jnp.where(ratio < 1.0, polynom, 0.0)
    kernel = tapered * (square * radius + target[4][..., :, None] * source[4][..., None, :]) ** (-1.0 / 3.0)
    return lax.optimization_barrier(jnp.sum(kernel * source[3][..., None, :], axis=-1))

def reference(offsets, history, occupied, species, chi_table, eta_table, gamma_table):
    weight = occupied.astype(jnp.float32)
    predicted = extrapolate_weights[0] * history[0]
    for level in range(1, 6):
        predicted = predicted + extrapolate_weights[level] * history[level]
    predicted = weight * predicted
    chi = lookup(species, chi_table)
    eta = lookup(species, eta_table)
    gam = lookup(species, gamma_table)
    shield = gam ** (-1.5)
    fields = jnp.concatenate([offsets, predicted[None], shield[None]], axis=0)
    target = jnp.moveaxis(fields, 1, 0)
    summed = jnp.zeros(predicted.shape, jnp.float32)
    for offset_index in range(27):
        step_x = offset_index // 9 - 1
        step_y = offset_index // 3 % 3 - 1
        step_z = offset_index % 3 - 1
        source = jnp.moveaxis(jnp.roll(fields, (-step_x, -step_y, -step_z), axis=(1, 2, 3)), 1, 0)
        shifts = (step_x * EDGE, step_y * EDGE, step_z * EDGE)
        summed = summed + lax.map(lambda couple: pair_sum(couple[0], couple[1], shifts), (target, source))
    potential = COULOMB * (summed - (shield * shield) ** (-1.0 / 3.0) * predicted)
    electroneg = chi + eta * predicted + potential
    atom_count = jnp.sum(weight)
    chem_potential = jnp.sum(weight * electroneg) / atom_count
    stepped = weight * (predicted - (electroneg - chem_potential) / eta)
    charge = weight * (stepped - jnp.sum(stepped) / atom_count)
    residual = weight * (electroneg - chem_potential)
    return (charge, residual)
```

```python
import math

import jax
import jax.numpy as jnp
import numpy as np
from jax import lax
from jax.experimental import pallas as pl
from jax.experimental.pallas import tpu as pltpu
from jax.sharding import PartitionSpec as P

EDGE = 10.0
COULOMB = 14.4
WEIGHTS = (22.0 / 7.0, -55.0 / 14.0, 55.0 / 21.0, -22.0 / 21.0, 5.0 / 21.0, -1.0 / 42.0)
FIELDS = 8
SHELL = [(a, 1, c) for a in (-1, 0, 1) for c in (-1, 0, 1)]
SHELL += [(a, 0, 1) for a in (-1, 0, 1)] + [(1, 0, 0)]
NP = len(SHELL)
F32 = jnp.float32
BF16 = jnp.bfloat16


def ring(n, k):
    return [(i, (i + k) % n) for i in range(n)]


def pieces_of(x):
    hi = x.astype(BF16)
    rest = x - hi.astype(F32)
    mid = rest.astype(BF16)
    low = (rest - mid.astype(F32)).astype(BF16)
    return hi, mid, low


def pick(species, table_ref):
    out = jnp.full(species.shape, table_ref[0], F32)
    for t in range(1, table_ref.shape[0]):
        out = jnp.where(species == t, table_ref[t], out)
    return out


def pack_kernel(off_ref, hist_ref, occ_ref, spec_ref, chi_ref, eta_ref, gam_ref, cell_ref, aux_ref, part_ref):
    cells, slots = occ_ref.shape
    weight = occ_ref[...].astype(F32)
    species = spec_ref[...]
    predicted = WEIGHTS[0] * hist_ref[0]
    for level in range(1, len(WEIGHTS)):
        predicted = predicted + WEIGHTS[level] * hist_ref[level]
    predicted = weight * predicted
    chi = pick(species, chi_ref)
    eta = pick(species, eta_ref)
    gam = pick(species, gam_ref)
    root = lax.rsqrt(gam)
    shield = root * root * root * (EDGE**-1.5)
    inverse = 1.0 / eta
    base = chi + eta * predicted - COULOMB * gam * predicted
    winv = weight * inverse
    zero = jnp.zeros((1, slots), F32)
    rows = [weight, weight * base, predicted, winv * base, winv]
    rows = [jnp.sum(r, axis=0, keepdims=True) for r in rows] + [zero] * 3
    part_ref[...] = jnp.concatenate(rows, axis=0)
    tri = lax.broadcasted_iota(jnp.int32, (slots, slots), 0) <= lax.broadcasted_iota(jnp.int32, (slots, slots), 1)
    wb = weight.astype(BF16)
    rank = jnp.dot(wb, tri.astype(F32).astype(BF16), preferred_element_type=F32)
    count = jnp.dot(wb, jnp.ones((slots, slots), BF16), preferred_element_type=F32)
    pos = jnp.where(weight > 0, rank - 1.0, -1.0)
    aux_ref[0] = base
    aux_ref[1] = predicted
    aux_ref[2] = inverse
    aux_ref[3] = pos
    fields = [off_ref[d] * (1.0 / EDGE) for d in range(3)] + [predicted, shield, winv, weight, weight]
    row_id = lax.broadcasted_iota(jnp.int32, (slots, slots), 0).astype(F32)
    lane = lax.broadcasted_iota(jnp.int32, (FIELDS, slots), 1).astype(F32)
    sub = lax.broadcasted_iota(jnp.int32, (FIELDS, slots), 0)
    for c in range(cells):
        feat = jnp.concatenate([f[c : c + 1] for f in fields], axis=0)
        hot = jnp.where(row_id == pos[c : c + 1], 1.0, 0.0).astype(BF16)
        parts = jnp.concatenate(pieces_of(feat), axis=0)
        out = lax.dot_general(parts, hot, (((1,), (1,)), ((), ())), preferred_element_type=F32)
        out = out[:FIELDS] + out[FIELDS : 2 * FIELDS] + out[2 * FIELDS :]
        number = jnp.broadcast_to(count[c : c + 1], (FIELDS, slots))
        out = jnp.where((sub == 4) & (lane >= number), 1.0, out)
        cell_ref[c] = jnp.where(sub == 7, number, out)


def pair_kernel(nb, z2, slots, chunk_ref, table_ref, part_ref, *refs):
    planes = refs[:-5]
    out_ref, abc, bbc, acca, accb = refs[-5:]
    nx = len(planes)
    r2 = planes[0].shape[0]
    per = r2 * z2
    nck = slots // 8
    nb1 = nb + 1
    ty, tz = r2 - 1, z2 - 2
    own = [(p, r, z) for p in range(nx) for r in range(ty) for z in range(tz)]
    cell_of = lambda p, r, z: p * per + r * z2 + z
    order = (0, 1, 2, 4, 3)
    for p in range(nx):
        for r in range(r2):
            for z in range(z2):
                cell = planes[p][r, z]
                for k, f in enumerate(order):
                    abc[cell_of(p, r, z), k] = jnp.broadcast_to(cell[f : f + 1], (8, slots))
    for b, (p, r, z) in enumerate(own):
        cell = planes[p][r, z + 1]
        turned = cell.T
        for k, f in enumerate(order):
            wide = jnp.broadcast_to(turned[:, f : f + 1], (slots, slots))
            bbc[b * nck : (b + 1) * nck, k] = wide.reshape(nck, 8, slots)
    blank = jnp.zeros((8, slots), F32)
    for k in range(5):
        bbc[nb * nck, k] = jnp.full((8, slots), 1.0 if k == 3 else 0.0, F32)
    for b in range(nb1):
        for s in range(2):
            for q in range(NP):
                acca[s, b, q] = blank
    for i in range(nb * nck):
        accb[i] = blank

    def value(ai, shift, bf):
        a, y, c = shift
        dx = abc[ai, 0] - bf[0][a]
        dy = abc[ai, 1] - bf[1][y]
        dz = abc[ai, 2] - bf[2][c]
        s = dx * dx + dy * dy + dz * dz
        s = jnp.minimum(jnp.maximum(s, 1e-12), 1.0)
        u = s * lax.rsqrt(s)
        v = 1.0 - u
        v = v * v
        v = v * v
        poly = ((u + 0.5) * u + 0.2) * u + 0.05
        x = s * u + abc[ai, 3] * bf[3]
        return (v * poly) * jnp.exp2(jnp.log2(x) * (-1.0 / 3.0))

    def item(slot, b, c):
        be = jnp.minimum(b, nb - 1)
        bases = [table_ref[a * nb1 + be] for a in range(3)]
        ci = jnp.where(b < nb, b * nck + c, nb * nck)
        raw = [bbc[ci, k] for k in range(5)]
        bf = [{o: (raw[k] - float(o) if o else raw[k]) for o in (-1, 0, 1)} for k in range(3)] + [raw[3]]
        qb = raw[4]
        k = value(bases[1], (0, 0, 0), bf)
        total = k * abc[bases[1], 4]
        for q, (a, y, z) in enumerate(SHELL):
            ai = bases[a + 1] + (y * z2 + z)
            k = value(ai, (a, y, z), bf)
            total = total + k * abc[ai, 4]
            acca[slot, b, q] = acca[slot, b, q] + k * qb
        accb[ci] = total

    def advance(b, c):
        more = c + 1 < chunk_ref[b]
        return jnp.where(more, b, jnp.minimum(b + 1, nb)), jnp.where(more, c + 1, 0)

    def step(_, carry):
        b, c = carry
        item(0, b, c)
        b, c = advance(b, c)
        item(1, b, c)
        return advance(b, c)

    lax.fori_loop(0, chunk_ref[nb1], step, (jnp.int32(0), jnp.int32(0)))

    sums = {}
    for b, (p, r, z) in enumerate(own):
        rows = accb[b * nck : (b + 1) * nck].reshape(slots, slots).T
        folded = rows[:8]
        for i in range(1, nck):
            folded = folded + rows[8 * i : 8 * i + 8]
        key = cell_of(p, r, z + 1)
        sums[key] = sums[key] + folded if key in sums else folded
        for q, (a, y, c) in enumerate(SHELL):
            key = cell_of((p + a) % nx, r + y, z + 1 + c)
            term = acca[0, b, q] + acca[1, b, q]
            sums[key] = sums[key] + term if key in sums else term
    one = jnp.zeros((1, slots), F32)
    two = jnp.zeros((1, slots), F32)
    for p in range(nx):
        for r in range(r2):
            for z in range(z2):
                key = cell_of(p, r, z)
                if key in sums:
                    row = jnp.sum(sums[key], axis=0, keepdims=True)
                    cell = planes[p][r, z]
                    one = one + cell[6:7] * row
                    two = two + cell[5:6] * row
                else:
                    row = jnp.zeros((1, slots), F32)
                out_ref[p, r * z2 + z : r * z2 + z + 1, :] = row
    scale = 2.0 * COULOMB
    part = part_ref[...]
    tail = jnp.concatenate([part[0:1], part[1:2] + scale * one, part[2:3], part[3:4] + scale * two, part[4:8]], axis=0)
    for p in range(nx):
        out_ref[p, per : per + 8, :] = tail


def finish_kernel(sum_ref, aux_ref, occ_ref, part_ref, charge_ref, resid_ref):
    cells, slots = occ_ref.shape
    weight = occ_ref[...].astype(F32)
    row_id = lax.broadcasted_iota(jnp.int32, (slots, slots), 0).astype(F32)
    packed = sum_ref[...]
    pos = aux_ref[3]
    hi, mid, low = [t.astype(F32) for t in pieces_of(packed)]
    lines = []
    for c in range(cells):
        hot = jnp.where(row_id == pos[c : c + 1], 1.0, 0.0).astype(BF16)
        parts = jnp.concatenate([hi[c : c + 1], mid[c : c + 1], low[c : c + 1]] + [jnp.zeros((5, slots), F32)], axis=0)
        out = jnp.dot(parts.astype(BF16), hot, preferred_element_type=F32)
        lines.append(out[0:1] + out[1:2] + out[2:3])
    summed = jnp.concatenate(lines, axis=0)
    totals = jnp.sum(part_ref[...], axis=1, keepdims=True)
    number, elec, charge_sum, scaled, inv_sum = [totals[i : i + 1] for i in range(5)]
    chem = elec / number
    stepped_total = charge_sum - scaled + chem * inv_sum
    delta = aux_ref[0] + (2.0 * COULOMB) * summed - chem
    stepped = weight * (aux_ref[1] - delta * aux_ref[2])
    charge_ref[...] = weight * (stepped - stepped_total / number)
    resid_ref[...] = weight * delta


def body(offsets, history, occupied, species, chi_table, eta_table, gamma_table):
    _, ny, nz, slots = occupied.shape
    cells = ny * nz
    nx, gy, gz = lax.axis_size("gx"), lax.axis_size("gy"), lax.axis_size("gz")
    py = math.gcd(nx, ny)
    pz = nx // py
    ty, tz = ny // py, nz // pz
    r2, z2 = ty + 1, tz + 2
    per = r2 * z2
    nb = nx * ty * tz
    nck = slots // 8
    vmem = pl.BlockSpec(memory_space=pltpu.VMEM)
    smem = pl.BlockSpec(memory_space=pltpu.SMEM)
    shape = lambda *s: jax.ShapeDtypeStruct(s, F32)
    occ = occupied.reshape(cells, slots)
    packed, aux, part = pl.pallas_call(
        pack_kernel,
        out_shape=(shape(cells, FIELDS, slots), shape(4, cells, slots), shape(8, slots)),
        in_specs=[vmem] * 4 + [smem] * 3,
        out_specs=(vmem, vmem, vmem),
        name="pack",
    )(
        offsets.reshape(3, cells, slots),
        history.reshape(-1, cells, slots),
        occ,
        species.reshape(cells, slots),
        chi_table,
        eta_table,
        gamma_table,
    )
    plane = packed.reshape(ny, nz, FIELDS, slots)
    low = lax.ppermute(plane[:, nz - 1 :], "gz", ring(gz, 1))
    high = lax.ppermute(plane[:, :1], "gz", ring(gz, -1))
    plane = jnp.concatenate([low, plane, high], axis=1)
    above = lax.ppermute(plane[:1], "gy", ring(gy, -1))
    plane = jnp.concatenate([plane, above], axis=0)
    me = lax.axis_index("gx")

    def tile(owner):
        return lax.dynamic_slice(plane, ((owner // pz) * ty, (owner % pz) * tz, 0, 0), (r2, z2, FIELDS, slots))

    planes = [tile(me)]
    for k in range(1, nx):
        planes.append(lax.ppermute(tile((me - k) % nx), "gx", ring(nx, -k)))
    number = jnp.stack([p[:ty, 1 : tz + 1, 7, 0] for p in planes]).reshape(nb).astype(jnp.int32)
    chunks = (number + 7) // 8
    steps = (jnp.sum(chunks) + 1) // 2
    chunks = jnp.concatenate([chunks, jnp.zeros((1,), jnp.int32), steps[None]])
    table = np.zeros((3, nb + 1), np.int32)
    for b in range(nb):
        p, r, z = b // (ty * tz), b // tz % ty, b % tz
        for a in range(3):
            table[a, b] = ((p + a - 1) % nx) * per + r * z2 + z + 1
    ncell = nx * per
    out = pl.pallas_call(
        lambda *refs: pair_kernel(nb, z2, slots, *refs),
        out_shape=shape(nx, per + 8, slots),
        in_specs=[smem, smem, vmem] + [vmem] * nx,
        out_specs=vmem,
        scratch_shapes=[
            pltpu.VMEM((ncell, 5, 8, slots), F32),
            pltpu.VMEM((nb * nck + 1, 5, 8, slots), F32),
            pltpu.VMEM((2, nb + 1, NP, 8, slots), F32),
            pltpu.VMEM((nb * nck + 1, 8, slots), F32),
        ],
        compiler_params=pltpu.CompilerParams(vmem_limit_bytes=40 * 1024 * 1024),
        name="pairs",
    )(chunks, jnp.asarray(table.reshape(-1)), part, *planes)
    gathered = [out[0]]
    for k in range(1, nx):
        gathered.append(lax.ppermute(out[k], "gx", ring(nx, k)))
    total = sum(g[per:] for g in gathered[1:]) + gathered[0][per:]
    wide = jnp.zeros((ny + 1, nz + 2, slots), F32)
    for k in range(nx):
        owner = (me - k) % nx
        at = ((owner // pz) * ty, (owner % pz) * tz, 0)
        piece = gathered[k][:per].reshape(r2, z2, slots)
        wide = wide + lax.dynamic_update_slice(jnp.zeros_like(wide), piece, at)
    total = total + lax.ppermute(total, "gz", ring(gz, 1)) if gz == 2 else lax.psum(total, "gz")
    back = lax.ppermute(wide[ny:], "gy", ring(gy, 1))
    if gy == 4:
        total = total + lax.ppermute(total, "gy", [(i, i ^ 1) for i in range(gy)])
        total = total + lax.ppermute(total, "gy", [(i, i ^ 2) for i in range(gy)])
    else:
        total = lax.psum(total, "gy")
    wide = jnp.concatenate([wide[:1] + back, wide[1:ny]], axis=0)
    from_high = lax.ppermute(wide[:, :1], "gz", ring(gz, -1))
    from_low = lax.ppermute(wide[:, nz + 1 :], "gz", ring(gz, 1))
    inner = wide[:, 1 : nz + 1]
    inner = jnp.concatenate([inner[:, :1] + from_low, inner[:, 1 : nz - 1], inner[:, nz - 1 :] + from_high], axis=1)
    charge, residual = pl.pallas_call(
        finish_kernel,
        out_shape=(shape(cells, slots), shape(cells, slots)),
        in_specs=[vmem] * 4,
        out_specs=(vmem, vmem),
        name="finish",
    )(inner.reshape(cells, slots), aux, occ, total)
    return charge.reshape(occupied.shape), residual.reshape(occupied.shape)


def solution(mesh):
    return jax.shard_map(
        body,
        mesh=mesh,
        in_specs=(
            P(None, "gx", "gy", "gz", None),
            P(None, "gx", "gy", "gz", None),
            P("gx", "gy", "gz", None),
            P("gx", "gy", "gz", None),
            P(),
            P(),
            P(),
        ),
        out_specs=(P("gx", "gy", "gz", None), P("gx", "gy", "gz", None)),
        check_vma=False,
    )
```

```python
import math

import jax
import jax.numpy as jnp
from jax import lax
from jax.experimental import pallas as pl
from jax.experimental.pallas import tpu as pltpu
from jax.sharding import PartitionSpec as P

EDGE = 10.0
COULOMB = 14.4
WEIGHTS = (22.0 / 7.0, -55.0 / 14.0, 55.0 / 21.0, -22.0 / 21.0, 5.0 / 21.0, -1.0 / 42.0)
FIELDS = 8
SHELL_UP = [(a, 1, c) for a in (-1, 0, 1) for c in (-1, 0, 1)]
SHELL_ROW = [(a, 0, 1) for a in (-1, 0, 1)] + [(1, 0, 0)]
UP_GROUP, ROW_GROUP = 3, 5
VMEM_LIMIT = 24 * 1024 * 1024
F32 = jnp.float32
BF16 = jnp.bfloat16


def ring(n, k):
    return [(i, (i + k) % n) for i in range(n)]


def pieces_of(x):
    hi = x.astype(BF16)
    rest = x - hi.astype(F32)
    mid = rest.astype(BF16)
    low = (rest - mid.astype(F32)).astype(BF16)
    return hi, mid, low


def pick(species, table_ref):
    out = jnp.full(species.shape, table_ref[0], F32)
    for t in range(1, table_ref.shape[0]):
        out = jnp.where(species == t, table_ref[t], out)
    return out


def pack_kernel(pz, tz, off_ref, hist_ref, occ_ref, spec_ref, chi_ref, eta_ref, gam_ref, aux_ref, part_ref, *refs):
    tiles, cell_ref = refs[:-1], refs[-1]
    cells, slots = occ_ref.shape
    weight = occ_ref[...].astype(F32)
    species = spec_ref[...]
    predicted = WEIGHTS[0] * hist_ref[0]
    for level in range(1, len(WEIGHTS)):
        predicted = predicted + WEIGHTS[level] * hist_ref[level]
    predicted = weight * predicted
    chi = pick(species, chi_ref)
    eta = pick(species, eta_ref)
    gam = pick(species, gam_ref)
    root = lax.rsqrt(gam)
    shield = root * root * root * (EDGE**-1.5)
    inverse = 1.0 / eta
    base = chi + eta * predicted - COULOMB * gam * predicted
    winv = weight * inverse
    zero = jnp.zeros((1, slots), F32)
    rows = [weight, weight * base, predicted, winv * base, winv]
    rows = [jnp.sum(r, axis=0, keepdims=True) for r in rows] + [zero] * 3
    part_ref[...] = jnp.concatenate(rows, axis=0)
    tri = lax.broadcasted_iota(jnp.int32, (slots, slots), 0) <= lax.broadcasted_iota(jnp.int32, (slots, slots), 1)
    wb = weight.astype(BF16)
    rank = jnp.dot(wb, tri.astype(F32).astype(BF16), preferred_element_type=F32)
    count = jnp.dot(wb, jnp.ones((slots, slots), BF16), preferred_element_type=F32)
    pos = jnp.where(weight > 0, rank - 1.0, -1.0)
    aux_ref[0] = base
    aux_ref[1] = predicted
    aux_ref[2] = inverse
    aux_ref[3] = pos
    fields = [off_ref[d] * (1.0 / EDGE) for d in range(3)] + [predicted, shield, winv, weight, weight]
    row_id = lax.broadcasted_iota(jnp.int32, (slots, slots), 0).astype(F32)
    lane = lax.broadcasted_iota(jnp.int32, (FIELDS, slots), 1).astype(F32)
    sub = lax.broadcasted_iota(jnp.int32, (FIELDS, slots), 0)
    for c in range(cells):
        feat = jnp.concatenate([f[c : c + 1] for f in fields], axis=0)
        hot = jnp.where(row_id == pos[c : c + 1], 1.0, 0.0).astype(BF16)
        parts = jnp.concatenate(pieces_of(feat), axis=0)
        out = lax.dot_general(parts, hot, (((1,), (1,)), ((), ())), preferred_element_type=F32)
        out = out[:FIELDS] + out[FIELDS : 2 * FIELDS] + out[2 * FIELDS :]
        number = jnp.broadcast_to(count[c : c + 1], (FIELDS, slots))
        out = jnp.where((sub == 4) & (lane >= number), 1.0, out)
        cell_ref[c] = jnp.where(sub == 7, number, out)
    nx = len(tiles)
    me = lax.axis_index("gx")
    ty = tiles[0].shape[0]
    nz = tz * pz
    for k in range(nx):
        owner = lax.rem(me + (nx - k), nx)
        corner = (owner // pz) * (ty * nz) + (owner % pz) * tz
        for r in range(ty):
            for z in range(tz):
                tiles[k][r, z] = cell_ref[corner + (r * nz + z)]


def pair_kernel(cfg, *refs):
    nx, ty, tz, slots = cfg["nx"], cfg["ty"], cfg["tz"], cfg["slots"]
    shell, alone, group = cfg["shell"], cfg["alone"], cfg["group"]
    side, up, first = cfg["side"], cfg["up"], cfg["first"]
    refs = list(refs)
    planes = [refs.pop(0) for _ in range(nx)]
    edge_low, edge_high = (refs.pop(0), refs.pop(0)) if side else (None, None)
    above = refs.pop(0) if up else None
    before = None if first else refs.pop(0)
    part_ref = refs.pop(0)
    out_ref, part_out = refs.pop(0), refs.pop(0)
    up_ref = refs.pop(0) if up else None
    abc, turned_ref, wide_ref, acca, accb, base_s, chunk_s, itemb_s, itemc_s = refs
    nck = slots // 8
    nb = nx * ty * len(cfg["mine"])
    z2 = tz + 2
    per = (ty + 1) * z2
    own = [(p, r, z) for p in range(nx) for r in range(ty) for z in cfg["mine"]]

    def cell_of(p, r, z):
        return (p % nx) * per + r * z2 + z + 1

    def load(p, r, z):
        if r < ty:
            return planes[p][r, z] if 0 <= z < tz else (edge_low[p, r] if z < 0 else edge_high[p, r])
        return above[(p - cfg["turn"]) % nx, z + 1]

    order = (0, 1, 2, 4, 3)
    total_chunks = jnp.int32(0)
    for b, (p, r, z) in enumerate(own):
        cell = load(p, r, z)
        turned_ref[b * nck : (b + 1) * nck] = cell.T.reshape(nck, 8, FIELDS)
        number = (jnp.max(cell[7:8]).astype(jnp.int32) + 7) // 8
        chunk_s[b] = number
        total_chunks = total_chunks + number
        for a in range(3):
            base_s[a * (nb + 1) + b] = cell_of(p + a - 1, r, z)
    chunk_s[nb] = 0
    for a in range(3):
        base_s[a * (nb + 1) + nb] = cell_of(0, 0, own[0][2])
    sub = lax.broadcasted_iota(jnp.int32, (8, slots), 0)
    slant = lax.broadcasted_iota(jnp.int32, (8, slots), 1) - sub
    blank = jnp.zeros((8, slots), F32)
    turned_ref[nb * nck] = jnp.where(lax.broadcasted_iota(jnp.int32, (8, FIELDS), 1) == 4, 1.0, 0.0)
    touched = {}
    for b, (p, r, z) in enumerate(own):
        for a, y, c in shell + ([(0, 0, 0)] if alone else []):
            touched[cell_of(p + a, r + y, z + c)] = ((p + a) % nx, r + y, z + c)
    for key, where in touched.items():
        cell = load(*where)
        for k, f in enumerate(order):
            abc[key, k] = jnp.broadcast_to(cell[f : f + 1], (8, slots))
    for b in range(nb + 1):
        for g in range(group):
            for q in range(len(shell)):
                acca[g, b, q] = blank

    def extend(t, b, c):
        for g in range(group):
            itemb_s[t * group + g] = b
            itemc_s[t * group + g] = c
            more = c + 1 < chunk_s[b]
            b, c = jnp.where(more, b, jnp.minimum(b + 1, nb)), jnp.where(more, c + 1, 0)
        return b, c

    def listed(t, g):
        return itemb_s[t * group + g], itemc_s[t * group + g]

    def prepare(t, g):
        b, c = listed(t, g)
        block = turned_ref[b * nck + c]
        for k, f in enumerate(order):
            wide_ref[g, k] = jnp.broadcast_to(block[:, f : f + 1], (8, slots))

    def value(ai, shift, bf):
        dx, dy, dz = [abc[ai, k] - bf[k][o] for k, o in enumerate(shift)]
        s = dx * dx + dy * dy + dz * dz
        s = jnp.minimum(jnp.maximum(s, 1e-12), 1.0)
        u = s * lax.rsqrt(s)
        v = 1.0 - u
        v = v * v
        v = v * v
        poly = ((u + 0.5) * u + 0.2) * u + 0.05
        x = s * u + abc[ai, 3] * bf[3]
        return (v * poly) * jnp.exp2(jnp.log2(x) * (-1.0 / 3.0))

    def item(t, g):
        b, c = listed(t, g)
        bases = [base_s[a * (nb + 1) + b] for a in range(3)]
        raw = [wide_ref[g, k] for k in range(5)]
        bf = [{o: (raw[k] - float(o) if o else raw[k]) for o in (-1, 0, 1)} for k in range(3)] + [raw[3]]
        qb = raw[4]
        total = None
        if alone:
            total = value(bases[1], (0, 0, 0), bf) * abc[bases[1], 4]
        for q, (a, y, z) in enumerate(shell):
            ai = bases[a + 1] + (y * z2 + z)
            k = value(ai, (a, y, z), bf)
            term = k * abc[ai, 4]
            total = term if total is None else total + term
            acca[g, b, q] = acca[g, b, q] + k * qb
        accb[b * nck + c] = total

    def step(t, carry):
        for g in range(group):
            item(t, g)
        for g in range(group):
            prepare(t + 1, g)
        return extend(t + 2, *carry)

    ahead = extend(1, *extend(0, jnp.int32(0), jnp.int32(0)))
    for g in range(group):
        prepare(0, g)
    steps = (total_chunks + (group - 1)) // group
    lax.fori_loop(0, steps, step, ahead)

    sums = {}

    def add(key, term):
        sums[key] = sums[key] + term if key in sums else term

    for b, (p, r, z) in enumerate(own):
        rows = accb[b * nck : (b + 1) * nck].reshape(slots, slots).T
        folded = rows[:8]
        for i in range(1, nck):
            folded = folded + rows[8 * i : 8 * i + 8]
        filled = jnp.broadcast_to(load(p, r, z)[6:7], (8, slots)) > 0.0
        add(cell_of(p, r, z), jnp.where(filled, folded, 0.0))
        for g in range(group):
            for q, (a, y, c) in enumerate(shell):
                add(cell_of(p + a, r + y, z + c), acca[g, b, q])
    one = jnp.zeros((1, slots), F32)
    two = jnp.zeros((1, slots), F32)
    for p in range(nx):
        for r in range(ty + 1):
            for z in range(-1, tz + 1):
                key = cell_of(p, r, z)
                row = jnp.zeros((1, slots), F32)
                if key in sums:
                    row = jnp.sum(sums[key], axis=0, keepdims=True)
                    cell = load(p, r, z)
                    one = one + cell[6:7] * row
                    two = two + cell[5:6] * row
                i = r * z2 + z + 1
                if r == ty:
                    if up:
                        up_ref[(p - cfg["turn"]) % nx, z + 1 : z + 2, :] = row
                elif first:
                    out_ref[p, i : i + 1, :] = row
                else:
                    out_ref[p, i : i + 1, :] = before[p, i : i + 1, :] + row
    scale = 2.0 * COULOMB
    part = part_ref[...]
    rows = [part[0:1], part[1:2] + scale * one, part[2:3], part[3:4] + scale * two, part[4:8]]
    rows = jnp.concatenate(rows, axis=0)
    if cfg["last"]:
        rows = jnp.broadcast_to(jnp.sum(rows, axis=1, keepdims=True), rows.shape)
    part_out[...] = rows


def pair_call(cfg, *args):
    nx, ty, tz, slots = cfg["nx"], cfg["ty"], cfg["tz"], cfg["slots"]
    nb = nx * ty * len(cfg["mine"])
    nck = slots // 8
    shape = lambda *s: jax.ShapeDtypeStruct(s, F32)
    vmem = pl.BlockSpec(memory_space=pltpu.VMEM)
    outs = [shape(nx, ty * (tz + 2), slots), shape(8, slots)]
    if cfg["up"]:
        outs.append(shape(nx, tz + 2, slots))
    return pl.pallas_call(
        lambda *refs: pair_kernel(cfg, *refs),
        out_shape=tuple(outs),
        in_specs=[vmem] * len(args),
        out_specs=(vmem,) * len(outs),
        scratch_shapes=[
            pltpu.VMEM((nx * (ty + 1) * (tz + 2), 5, 8, slots), F32),
            pltpu.VMEM((nb * nck + 1, 8, FIELDS), F32),
            pltpu.VMEM((cfg["group"], 5, 8, slots), F32),
            pltpu.VMEM((cfg["group"], nb + 1, len(cfg["shell"]), 8, slots), F32),
            pltpu.VMEM((nb * nck + 1, 8, slots), F32),
            pltpu.SMEM((3 * (nb + 1),), jnp.int32),
            pltpu.SMEM((nb + 1,), jnp.int32),
            pltpu.SMEM((nb * nck + 4 * cfg["group"],), jnp.int32),
            pltpu.SMEM((nb * nck + 4 * cfg["group"],), jnp.int32),
        ],
        compiler_params=pltpu.CompilerParams(vmem_limit_bytes=VMEM_LIMIT),
        name=cfg["name"],
    )(*args)


def unpack_kernel(sum_ref, aux_ref, out_ref):
    cells, slots = out_ref.shape
    row_id = lax.broadcasted_iota(jnp.int32, (slots, slots), 0).astype(F32)
    pos = aux_ref[3]
    hi, mid, low = [t.astype(F32) for t in pieces_of(sum_ref[...])]
    lines = []
    for c in range(cells):
        hot = jnp.where(row_id == pos[c : c + 1], 1.0, 0.0).astype(BF16)
        parts = jnp.concatenate([hi[c : c + 1], mid[c : c + 1], low[c : c + 1]] + [jnp.zeros((5, slots), F32)], axis=0)
        out = jnp.dot(parts.astype(BF16), hot, preferred_element_type=F32)
        lines.append(out[0:1] + out[1:2] + out[2:3])
    out_ref[...] = jnp.concatenate(lines, axis=0)


def body(offsets, history, occupied, species, chi_table, eta_table, gamma_table):
    _, ny, nz, slots = occupied.shape
    cells = ny * nz
    axes = ("gx", "gy", "gz")
    nx, gy, gz = [lax.axis_size(a) for a in axes]
    py = math.gcd(nx, ny)
    pz = nx // py
    ty, tz = ny // py, nz // pz
    z2 = tz + 2
    vmem = pl.BlockSpec(memory_space=pltpu.VMEM)
    shape = lambda *s: jax.ShapeDtypeStruct(s, F32)
    occ = occupied.reshape(cells, slots)
    aux, part, *tiles = pl.pallas_call(
        lambda *refs: pack_kernel(pz, tz, *refs),
        out_shape=(shape(4, cells, slots), shape(8, slots)) + (shape(ty, tz, FIELDS, slots),) * nx,
        in_specs=[vmem] * 4 + [pl.BlockSpec(memory_space=pltpu.SMEM)] * 3,
        out_specs=(vmem,) * (2 + nx),
        scratch_shapes=[pltpu.VMEM((cells, FIELDS, slots), F32)],
        name="pack",
    )(
        offsets.reshape(3, cells, slots),
        history.reshape(-1, cells, slots),
        occ,
        species.reshape(cells, slots),
        chi_table,
        eta_table,
        gamma_table,
    )
    me = lax.axis_index("gx")
    planes = [tiles[0]] + [lax.ppermute(tiles[k], "gx", ring(nx, -k)) for k in range(1, nx)]

    def number_of(x, y, z):
        return (x * gy + y) * gz + z

    def towards(up, side):
        pairs = []
        for x in range(nx):
            for y in range(gy):
                for z in range(gz):
                    row = (y * py + x // pz + up) % (gy * py)
                    col = (z * pz + x % pz + side) % (gz * pz)
                    pairs.append((number_of(row % py * pz + col % pz, row // py, col // pz), number_of(x, y, z)))
        return pairs

    def turned(array, side):
        if pz == 1:
            return array
        col = me % pz
        return jnp.roll(array, (col + side) % pz - col, axis=0)

    first = jnp.stack([p[:, 0] for p in planes])
    last = jnp.stack([p[:, tz - 1] for p in planes])
    if gz * pz == 2:
        both = lax.ppermute(jnp.stack([first, last]), axes, towards(0, 1))
        edge_low, edge_high = turned(both[1], -1), turned(both[0], 1)
    else:
        edge_low = turned(lax.ppermute(last, axes, towards(0, -1)), -1)
        edge_high = turned(lax.ppermute(first, axes, towards(0, 1)), 1)
    bottom = jnp.concatenate([edge_low[:, :1], jnp.stack([p[0] for p in planes]), edge_high[:, :1]], axis=1)
    above = lax.ppermute(bottom, axes, towards(1, 0))

    common = dict(nx=nx, ty=ty, tz=tz, slots=slots, turn=pz % nx)
    half = tz // 2
    row = dict(common, shell=SHELL_ROW, alone=True, group=ROW_GROUP, side=True, up=False)
    early = dict(row, name="early", mine=range(half), first=True, last=False)
    late = dict(row, name="late", mine=range(half, tz), first=False, last=True)
    upper = dict(common, name="upper", mine=range(tz), shell=SHELL_UP, alone=False, group=UP_GROUP, side=ty > 1, up=True, first=False, last=False)
    sums, part = pair_call(early, *planes, edge_low, edge_high, part)
    inner_edges = (edge_low, edge_high) if ty > 1 else ()
    sums, part, up_sums = pair_call(upper, *planes, *inner_edges, above, sums, part)
    back = lax.ppermute(up_sums, axes, [(t, s) for s, t in towards(1, 0)])
    sums, part = pair_call(late, *planes, edge_low, edge_high, sums, part)

    sums = jnp.concatenate([sums[:, :z2] + back, sums[:, z2:], jnp.broadcast_to(part, (nx,) + part.shape)], axis=1)
    rows = ty * z2
    gathered = [sums[0]] + [lax.ppermute(sums[k], "gx", ring(nx, k)) for k in range(1, nx)]
    total = gathered[0][rows:]
    for g in gathered[1:]:
        total = total + g[rows:]
    for axis, count in (("gz", gz), ("gy", gy)):
        if count & (count - 1):
            total = lax.psum(total, axis)
        else:
            for bit in range(count.bit_length() - 1):
                total = total + lax.ppermute(total, axis, [(i, i ^ (1 << bit)) for i in range(count)])
    wide = jnp.zeros((ny, nz + 2, slots), F32)
    for k in range(nx):
        owner = (me - k) % nx
        at = ((owner // pz) * ty, (owner % pz) * tz, 0)
        piece = gathered[k][:rows].reshape(ty, z2, slots)
        wide = wide + lax.dynamic_update_slice(jnp.zeros_like(wide), piece, at)
    if gz == 2:
        both = lax.ppermute(jnp.stack([wide[:, 0], wide[:, nz + 1]]), "gz", ring(gz, 1))
        from_high, from_low = both[0], both[1]
    else:
        from_high = lax.ppermute(wide[:, 0], "gz", ring(gz, -1))
        from_low = lax.ppermute(wide[:, nz + 1], "gz", ring(gz, 1))
    inner = wide[:, 1 : nz + 1]
    inner = jnp.concatenate(
        [inner[:, :1] + from_low[:, None], inner[:, 1 : nz - 1], inner[:, nz - 1 :] + from_high[:, None]], axis=1
    )
    summed = pl.pallas_call(
        unpack_kernel,
        out_shape=shape(cells, slots),
        in_specs=[vmem] * 2,
        out_specs=vmem,
        compiler_params=pltpu.CompilerParams(vmem_limit_bytes=VMEM_LIMIT),
        name="unpack",
    )(inner.reshape(cells, slots), aux)
    weight = occ.astype(F32)
    number, elec, charge_sum, scaled, inv_sum = [total[i : i + 1] for i in range(5)]
    chem = elec / number
    stepped_total = charge_sum - scaled + chem * inv_sum
    delta = aux[0] + (2.0 * COULOMB) * summed - chem
    stepped = weight * (aux[1] - delta * aux[2])
    charge = weight * (stepped - stepped_total / number)
    residual = weight * delta
    return charge.reshape(occupied.shape), residual.reshape(occupied.shape)


def solution(mesh):
    return jax.shard_map(
        body,
        mesh=mesh,
        in_specs=(
            P(None, "gx", "gy", "gz", None),
            P(None, "gx", "gy", "gz", None),
            P("gx", "gy", "gz", None),
            P("gx", "gy", "gz", None),
            P(),
            P(),
            P(),
        ),
        out_specs=(P("gx", "gy", "gz", None), P("gx", "gy", "gz", None)),
        check_vma=False,
    )
```

```python
import math

import jax
import jax.numpy as jnp
from jax import lax
from jax.experimental import pallas as pl
from jax.experimental.pallas import tpu as pltpu
from jax.sharding import PartitionSpec as P

EDGE = 10.0
COULOMB = 14.4
WEIGHTS = (22.0 / 7.0, -55.0 / 14.0, 55.0 / 21.0, -22.0 / 21.0, 5.0 / 21.0, -1.0 / 42.0)
FIELDS = 8
SHELL_UP = [(a, 1, c) for a in (-1, 0, 1) for c in (-1, 0, 1)]
SHELL_ROW = [(a, 0, 1) for a in (-1, 0, 1)] + [(1, 0, 0)]
UP_GROUP, ROW_GROUP = 3, 5


def real_root():
    u = -0.34
    for _ in range(8):
        u -= (((u + 0.5) * u + 0.2) * u + 0.05) / ((3.0 * u + 1.0) * u + 0.2)
    return -u


ROOT = real_root()
LINEAR = 0.5 - ROOT
FREE = 0.2 - ROOT * LINEAR
REACH = 1.0 / LINEAR
SCALE = 2.0 * COULOMB / REACH**6
VMEM_LIMIT = 24 * 1024 * 1024
F32 = jnp.float32
BF16 = jnp.bfloat16


def fold(g, n):
    if n % 2:
        return g
    half = n // 2
    return (3 * half - 1 - g if g >= half else g) if isinstance(g, int) else jnp.where(g < half, g, 3 * half - 1 - g)


def tile_of(g, y, n):
    t = fold(g, n)
    if isinstance(y, int):
        return n - 1 - t if y % 2 else t
    return jnp.where(lax.rem(y, 2) == 1, n - 1 - t, t)


def device_of(t, y, n):
    if isinstance(y, int):
        return fold(n - 1 - t if y % 2 else t, n)
    return fold(jnp.where(lax.rem(y, 2) == 1, n - 1 - t, t), n)


def ring(n, k):
    return [(i, (i + k) % n) for i in range(n)]


def pieces_of(x):
    hi = x.astype(BF16)
    rest = x - hi.astype(F32)
    mid = rest.astype(BF16)
    low = (rest - mid.astype(F32)).astype(BF16)
    return hi, mid, low


def pick(species, table_ref):
    out = jnp.full(species.shape, table_ref[0], F32)
    for t in range(1, table_ref.shape[0]):
        out = jnp.where(species == t, table_ref[t], out)
    return out


def pack_kernel(pz, tz, off_ref, hist_ref, occ_ref, spec_ref, chi_ref, eta_ref, gam_ref, aux_ref, part_ref, *refs):
    tiles, cell_ref = refs[:-1], refs[-1]
    cells, slots = occ_ref.shape
    weight = occ_ref[...].astype(F32)
    species = spec_ref[...]
    predicted = WEIGHTS[0] * hist_ref[0]
    for level in range(1, len(WEIGHTS)):
        predicted = predicted + WEIGHTS[level] * hist_ref[level]
    predicted = weight * predicted
    chi = pick(species, chi_ref)
    eta = pick(species, eta_ref)
    gam = pick(species, gam_ref)
    root = lax.rsqrt(gam)
    shield = root * root * root * ((REACH / EDGE) ** 1.5)
    inverse = 1.0 / eta
    base = chi + eta * predicted - COULOMB * gam * predicted
    winv = weight * inverse
    zero = jnp.zeros((1, slots), F32)
    rows = [weight, weight * base, predicted, winv * base, winv]
    rows = [jnp.sum(r, axis=0, keepdims=True) for r in rows] + [zero] * 3
    part_ref[...] = jnp.broadcast_to(jnp.sum(jnp.concatenate(rows, axis=0), axis=1, keepdims=True), part_ref.shape)
    tri = lax.broadcasted_iota(jnp.int32, (slots, slots), 0) <= lax.broadcasted_iota(jnp.int32, (slots, slots), 1)
    wb = weight.astype(BF16)
    rank = jnp.dot(wb, tri.astype(F32).astype(BF16), preferred_element_type=F32)
    count = jnp.dot(wb, jnp.ones((slots, slots), BF16), preferred_element_type=F32)
    pos = jnp.where(weight > 0, rank - 1.0, -1.0)
    aux_ref[0] = base
    aux_ref[1] = predicted
    aux_ref[2] = inverse
    aux_ref[3] = pos
    fields = [off_ref[d] * (REACH / EDGE) for d in range(3)] + [predicted, shield, winv, weight, weight]
    row_id = lax.broadcasted_iota(jnp.int32, (slots, slots), 0).astype(F32)
    lane = lax.broadcasted_iota(jnp.int32, (FIELDS, slots), 1).astype(F32)
    sub = lax.broadcasted_iota(jnp.int32, (FIELDS, slots), 0)
    for c in range(cells):
        feat = jnp.concatenate([f[c : c + 1] for f in fields], axis=0)
        hot = jnp.where(row_id == pos[c : c + 1], 1.0, 0.0).astype(BF16)
        parts = jnp.concatenate(pieces_of(feat), axis=0)
        out = lax.dot_general(parts, hot, (((1,), (1,)), ((), ())), preferred_element_type=F32)
        out = out[:FIELDS] + out[FIELDS : 2 * FIELDS] + out[2 * FIELDS :]
        number = jnp.broadcast_to(count[c : c + 1], (FIELDS, slots))
        out = jnp.where((sub == 4) & (lane >= number), 1.0, out)
        cell_ref[c] = jnp.where(sub == 7, number, out)
    nx = len(tiles)
    me = lax.axis_index("gx")
    ty = tiles[0].shape[0]
    nz = tz * pz
    for k in range(nx):
        owner = tile_of(lax.rem(me + (nx - k), nx), lax.axis_index("gy"), nx)
        corner = (owner // pz) * (ty * nz) + (owner % pz) * tz
        for r in range(ty):
            for z in range(tz):
                tiles[k][r, z] = cell_ref[corner + (r * nz + z)]


def pair_kernel(cfg, *refs):
    nx, ty, tz, slots = cfg["nx"], cfg["ty"], cfg["tz"], cfg["slots"]
    shell, alone, group = cfg["shell"], cfg["alone"], cfg["group"]
    side, up, first = cfg["side"], cfg["up"], cfg["first"]
    refs = list(refs)
    planes = [refs.pop(0) for _ in range(nx)]
    edge_low, edge_high = (refs.pop(0), refs.pop(0)) if side else (None, None)
    above = refs.pop(0) if up else None
    before, part_ref = (None, None) if first else (refs.pop(0), refs.pop(0))
    out_ref, part_out = refs.pop(0), refs.pop(0)
    up_ref = refs.pop(0) if up else None
    abc, turned_ref, wide_ref, acca, accb, base_s, chunk_s, itemb_s, itemc_s = refs
    nck = slots // 8
    if up:
        me, y = lax.axis_index("gx"), lax.axis_index("gy")
        t = tile_of(me, y, nx) + cfg["pz"]
        y = lax.rem(y + jnp.where(t < nx, 0, 1), cfg["gy"])
        turn = device_of(lax.rem(t, nx), y, nx) - me
        there = [lax.rem(p - turn + 2 * nx, nx) for p in range(nx)]
    nb = nx * ty * len(cfg["mine"])
    z2 = tz + 2
    per = (ty + 1) * z2
    own = [(p, r, z) for p in range(nx) for r in range(ty) for z in cfg["mine"]]

    def cell_of(p, r, z):
        return (p % nx) * per + r * z2 + z + 1

    def load(p, r, z):
        if r < ty:
            return planes[p][r, z] if 0 <= z < tz else (edge_low[p, r] if z < 0 else edge_high[p, r])
        return above[there[p], z + 1]

    order = (0, 1, 2, 4, 3)
    total_chunks = jnp.int32(0)
    for b, (p, r, z) in enumerate(own):
        cell = load(p, r, z)
        turned_ref[b * nck : (b + 1) * nck] = cell.T.reshape(nck, 8, FIELDS)
        number = (jnp.max(cell[7:8]).astype(jnp.int32) + 7) // 8
        chunk_s[b] = number
        total_chunks = total_chunks + number
        for a in range(3):
            base_s[a * (nb + 1) + b] = cell_of(p + a - 1, r, z)
    chunk_s[nb] = 0
    for a in range(3):
        base_s[a * (nb + 1) + nb] = cell_of(0, 0, own[0][2])
    sub = lax.broadcasted_iota(jnp.int32, (8, slots), 0)
    slant = lax.broadcasted_iota(jnp.int32, (8, slots), 1) - sub
    blank = jnp.zeros((8, slots), F32)
    turned_ref[nb * nck] = jnp.where(lax.broadcasted_iota(jnp.int32, (8, FIELDS), 1) == 4, 1.0, 0.0)
    touched = {}
    for b, (p, r, z) in enumerate(own):
        for a, y, c in shell + ([(0, 0, 0)] if alone else []):
            touched[cell_of(p + a, r + y, z + c)] = ((p + a) % nx, r + y, z + c)
    for key, where in touched.items():
        cell = load(*where)
        for k, f in enumerate(order):
            abc[key, k] = jnp.broadcast_to(cell[f : f + 1], (8, slots))
    for b in range(nb + 1):
        for g in range(group):
            for q in range(len(shell)):
                acca[g, b, q] = blank

    def extend(t, b, c):
        for g in range(group):
            itemb_s[t * group + g] = b
            itemc_s[t * group + g] = c
            more = c + 1 < chunk_s[b]
            b, c = jnp.where(more, b, jnp.minimum(b + 1, nb)), jnp.where(more, c + 1, 0)
        return b, c

    def listed(t, g):
        return itemb_s[t * group + g], itemc_s[t * group + g]

    def prepare(t, g):
        b, c = listed(t, g)
        block = turned_ref[b * nck + c]
        for k, f in enumerate(order):
            wide_ref[g, k] = jnp.broadcast_to(block[:, f : f + 1], (8, slots))

    def value(ai, shift, bf):
        dx, dy, dz = [abc[ai, k] - bf[k][o] for k, o in enumerate(shift)]
        s = dx * dx + dy * dy + dz * dz
        s = jnp.minimum(jnp.maximum(s, 1e-12), REACH * REACH)
        u = s * lax.rsqrt(s)
        v = REACH - u
        v = v * v
        v = v * v
        poly = (u + ROOT * REACH) * ((s + u) + FREE * REACH * REACH)
        x = s * u + abc[ai, 3] * bf[3]
        return (v * poly) * jnp.exp2(jnp.log2(x) * (-1.0 / 3.0))

    def item(t, g):
        b, c = listed(t, g)
        bases = [base_s[a * (nb + 1) + b] for a in range(3)]
        raw = [wide_ref[g, k] for k in range(5)]
        bf = [{o: (raw[k] - o * REACH if o else raw[k]) for o in (-1, 0, 1)} for k in range(3)] + [raw[3]]
        qb = raw[4]
        total = None
        if alone:
            total = value(bases[1], (0, 0, 0), bf) * abc[bases[1], 4]
        for q, (a, y, z) in enumerate(shell):
            ai = bases[a + 1] + (y * z2 + z)
            k = value(ai, (a, y, z), bf)
            term = k * abc[ai, 4]
            total = term if total is None else total + term
            acca[g, b, q] = acca[g, b, q] + k * qb
        accb[b * nck + c] = total

    def step(t, carry):
        for g in range(group):
            item(t, g)
        for g in range(group):
            prepare(t + 1, g)
        return extend(t + 2, *carry)

    ahead = extend(1, *extend(0, jnp.int32(0), jnp.int32(0)))
    for g in range(group):
        prepare(0, g)
    steps = (total_chunks + (group - 1)) // group
    lax.fori_loop(0, steps, step, ahead)

    sums = {}

    def add(key, term):
        sums[key] = sums[key] + term if key in sums else term

    for b, (p, r, z) in enumerate(own):
        rows = accb[b * nck : (b + 1) * nck].reshape(slots, slots).T
        folded = rows[:8]
        for i in range(1, nck):
            folded = folded + rows[8 * i : 8 * i + 8]
        filled = jnp.broadcast_to(load(p, r, z)[6:7], (8, slots)) > 0.0
        add(cell_of(p, r, z), jnp.where(filled, folded, 0.0))
        for g in range(group):
            for q, (a, y, c) in enumerate(shell):
                add(cell_of(p + a, r + y, z + c), acca[g, b, q])
    one = jnp.zeros((1, slots), F32)
    two = jnp.zeros((1, slots), F32)
    for p in range(nx):
        for r in range(ty + 1):
            for z in range(-1, tz + 1):
                key = cell_of(p, r, z)
                row = jnp.zeros((1, slots), F32)
                if key in sums:
                    row = jnp.sum(sums[key], axis=0, keepdims=True)
                    cell = load(p, r, z)
                    one = one + cell[6:7] * row
                    two = two + cell[5:6] * row
                i = r * z2 + z + 1
                if r == ty:
                    if up:
                        up_ref[there[p], z + 1 : z + 2, :] = row
                elif first:
                    out_ref[p, i : i + 1, :] = row
                else:
                    out_ref[p, i : i + 1, :] = before[p, i : i + 1, :] + row
    scale = SCALE
    none = jnp.zeros((1, slots), F32)
    rows = jnp.concatenate([none, scale * one, none, scale * two] + [none] * 4, axis=0)
    if not first:
        rows = rows + part_ref[...]
    if cfg["last"]:
        rows = jnp.broadcast_to(jnp.sum(rows, axis=1, keepdims=True), rows.shape)
    part_out[...] = rows


def pair_call(cfg, *args):
    nx, ty, tz, slots = cfg["nx"], cfg["ty"], cfg["tz"], cfg["slots"]
    nb = nx * ty * len(cfg["mine"])
    nck = slots // 8
    shape = lambda *s: jax.ShapeDtypeStruct(s, F32)
    vmem = pl.BlockSpec(memory_space=pltpu.VMEM)
    outs = [shape(nx, ty * (tz + 2), slots), shape(8, slots)]
    if cfg["up"]:
        outs.append(shape(nx, tz + 2, slots))
    return pl.pallas_call(
        lambda *refs: pair_kernel(cfg, *refs),
        out_shape=tuple(outs),
        in_specs=[vmem] * len(args),
        out_specs=(vmem,) * len(outs),
        scratch_shapes=[
            pltpu.VMEM((nx * (ty + 1) * (tz + 2), 5, 8, slots), F32),
            pltpu.VMEM((nb * nck + 1, 8, FIELDS), F32),
            pltpu.VMEM((cfg["group"], 5, 8, slots), F32),
            pltpu.VMEM((cfg["group"], nb + 1, len(cfg["shell"]), 8, slots), F32),
            pltpu.VMEM((nb * nck + 1, 8, slots), F32),
            pltpu.SMEM((3 * (nb + 1),), jnp.int32),
            pltpu.SMEM((nb + 1,), jnp.int32),
            pltpu.SMEM((nb * nck + 4 * cfg["group"],), jnp.int32),
            pltpu.SMEM((nb * nck + 4 * cfg["group"],), jnp.int32),
        ],
        compiler_params=pltpu.CompilerParams(vmem_limit_bytes=VMEM_LIMIT),
        name=cfg["name"],
    )(*args)


def unpack_kernel(sum_ref, aux_ref, out_ref):
    cells, slots = out_ref.shape
    row_id = lax.broadcasted_iota(jnp.int32, (slots, slots), 0).astype(F32)
    pos = aux_ref[3]
    hi, mid, low = [t.astype(F32) for t in pieces_of(sum_ref[...])]
    lines = []
    for c in range(cells):
        hot = jnp.where(row_id == pos[c : c + 1], 1.0, 0.0).astype(BF16)
        parts = jnp.concatenate([hi[c : c + 1], mid[c : c + 1], low[c : c + 1]] + [jnp.zeros((5, slots), F32)], axis=0)
        out = jnp.dot(parts.astype(BF16), hot, preferred_element_type=F32)
        lines.append(out[0:1] + out[1:2] + out[2:3])
    out_ref[...] = jnp.concatenate(lines, axis=0)


def body(offsets, history, occupied, species, chi_table, eta_table, gamma_table):
    _, ny, nz, slots = occupied.shape
    cells = ny * nz
    axes = ("gx", "gy", "gz")
    nx, gy, gz = [lax.axis_size(a) for a in axes]
    py = math.gcd(nx, ny)
    pz = nx // py
    ty, tz = ny // py, nz // pz
    z2 = tz + 2
    vmem = pl.BlockSpec(memory_space=pltpu.VMEM)
    shape = lambda *s: jax.ShapeDtypeStruct(s, F32)
    occ = occupied.reshape(cells, slots)
    aux, part, *tiles = pl.pallas_call(
        lambda *refs: pack_kernel(pz, tz, *refs),
        out_shape=(shape(4, cells, slots), shape(8, slots)) + (shape(ty, tz, FIELDS, slots),) * nx,
        in_specs=[vmem] * 4 + [pl.BlockSpec(memory_space=pltpu.SMEM)] * 3,
        out_specs=(vmem,) * (2 + nx),
        scratch_shapes=[pltpu.VMEM((cells, FIELDS, slots), F32)],
        name="pack",
    )(
        offsets.reshape(3, cells, slots),
        history.reshape(-1, cells, slots),
        occ,
        species.reshape(cells, slots),
        chi_table,
        eta_table,
        gamma_table,
    )
    me, column = lax.axis_index("gx"), lax.axis_index("gy")
    planes = [tiles[0]] + [lax.ppermute(tiles[k], "gx", ring(nx, -k)) for k in range(1, nx)]

    def number_of(x, y, z):
        return (x * gy + y) * gz + z

    def towards(up, side):
        pairs = []
        for x in range(nx):
            for y in range(gy):
                for z in range(gz):
                    t = tile_of(x, y, nx)
                    row = (y * py + t // pz + up) % (gy * py)
                    col = (z * pz + t % pz + side) % (gz * pz)
                    source = device_of(row % py * pz + col % pz, row // py, nx)
                    pairs.append((number_of(source, row // py, col // pz), number_of(x, y, z)))
        return pairs

    def turned(array, side):
        if pz == 1:
            return array
        t = tile_of(me, column, nx)
        t = t - t % pz + (t + side) % pz
        return jnp.roll(array, device_of(t, column, nx) - me, axis=0)

    first = jnp.stack([p[:, 0] for p in planes])
    last = jnp.stack([p[:, tz - 1] for p in planes])
    if gz * pz == 2:
        both = lax.ppermute(jnp.stack([first, last]), axes, towards(0, 1))
        edge_low, edge_high = turned(both[1], -1), turned(both[0], 1)
    else:
        edge_low = turned(lax.ppermute(last, axes, towards(0, -1)), -1)
        edge_high = turned(lax.ppermute(first, axes, towards(0, 1)), 1)
    bottom = jnp.concatenate([edge_low[:, :1], jnp.stack([p[0] for p in planes]), edge_high[:, :1]], axis=1)
    above = lax.ppermute(bottom, axes, towards(1, 0))

    common = dict(nx=nx, ty=ty, tz=tz, slots=slots, pz=pz, gy=gy)
    half = tz // 2
    row = dict(common, shell=SHELL_ROW, alone=True, group=ROW_GROUP, side=True, up=False)
    early = dict(row, name="early", mine=range(half), first=True, last=False)
    late = dict(row, name="late", mine=range(half, tz), first=False, last=True)
    upper = dict(common, name="upper", mine=range(tz), shell=SHELL_UP, alone=False, group=UP_GROUP, side=ty > 1, up=True, first=False, last=False)
    sums, found = pair_call(early, *planes, edge_low, edge_high)
    inner_edges = (edge_low, edge_high) if ty > 1 else ()
    sums, found, up_sums = pair_call(upper, *planes, *inner_edges, above, sums, found)
    back = lax.ppermute(up_sums, axes, [(t, s) for s, t in towards(1, 0)])
    sums, found = pair_call(late, *planes, edge_low, edge_high, sums, found)
    part = part + found

    sums = jnp.concatenate([sums[:, :z2] + back, sums[:, z2:], jnp.broadcast_to(part, (nx,) + part.shape)], axis=1)
    rows = ty * z2
    gathered = [sums[0]] + [lax.ppermute(sums[k], "gx", ring(nx, k)) for k in range(1, nx)]
    total = gathered[0][rows:]
    for g in gathered[1:]:
        total = total + g[rows:]
    for axis, count in (("gz", gz), ("gy", gy)):
        if count & (count - 1):
            total = lax.psum(total, axis)
        else:
            for bit in range(count.bit_length() - 1):
                total = total + lax.ppermute(total, axis, [(i, i ^ (1 << bit)) for i in range(count)])
    wide = jnp.zeros((ny, nz + 2, slots), F32)
    for k in range(nx):
        owner = tile_of((me - k) % nx, column, nx)
        at = ((owner // pz) * ty, (owner % pz) * tz, 0)
        piece = gathered[k][:rows].reshape(ty, z2, slots)
        wide = wide + lax.dynamic_update_slice(jnp.zeros_like(wide), piece, at)
    if gz == 2:
        both = lax.ppermute(jnp.stack([wide[:, 0], wide[:, nz + 1]]), "gz", ring(gz, 1))
        from_high, from_low = both[0], both[1]
    else:
        from_high = lax.ppermute(wide[:, 0], "gz", ring(gz, -1))
        from_low = lax.ppermute(wide[:, nz + 1], "gz", ring(gz, 1))
    inner = wide[:, 1 : nz + 1]
    inner = jnp.concatenate(
        [inner[:, :1] + from_low[:, None], inner[:, 1 : nz - 1], inner[:, nz - 1 :] + from_high[:, None]], axis=1
    )
    summed = pl.pallas_call(
        unpack_kernel,
        out_shape=shape(cells, slots),
        in_specs=[vmem] * 2,
        out_specs=vmem,
        compiler_params=pltpu.CompilerParams(vmem_limit_bytes=VMEM_LIMIT),
        name="unpack",
    )(inner.reshape(cells, slots), aux)
    weight = occ.astype(F32)
    number, elec, charge_sum, scaled, inv_sum = [total[i : i + 1] for i in range(5)]
    chem = elec / number
    stepped_total = charge_sum - scaled + chem * inv_sum
    delta = aux[0] + SCALE * summed - chem
    stepped = weight * (aux[1] - delta * aux[2])
    charge = weight * (stepped - stepped_total / number)
    residual = weight * delta
    return charge.reshape(occupied.shape), residual.reshape(occupied.shape)


def solution(mesh):
    return jax.shard_map(
        body,
        mesh=mesh,
        in_specs=(
            P(None, "gx", "gy", "gz", None),
            P(None, "gx", "gy", "gz", None),
            P("gx", "gy", "gz", None),
            P("gx", "gy", "gz", None),
            P(),
            P(),
            P(),
        ),
        out_specs=(P("gx", "gy", "gz", None), P("gx", "gy", "gz", None)),
        check_vma=False,
    )
```

```python
import math

import jax
import jax.numpy as jnp
from jax import lax
from jax.experimental import pallas as pl
from jax.experimental.pallas import tpu as pltpu
from jax.sharding import PartitionSpec as P

EDGE = 10.0
COULOMB = 14.4
WEIGHTS = (22.0 / 7.0, -55.0 / 14.0, 55.0 / 21.0, -22.0 / 21.0, 5.0 / 21.0, -1.0 / 42.0)
FIELDS = 8
SHELL_UP = [(a, 1, c) for a in (-1, 0, 1) for c in (-1, 0, 1)]
SHELL_ROW = [(a, 0, 1) for a in (-1, 0, 1)] + [(1, 0, 0)]
UP_GROUP, ROW_GROUP = 3, 8


def real_root():
    u = -0.34
    for _ in range(8):
        u -= (((u + 0.5) * u + 0.2) * u + 0.05) / ((3.0 * u + 1.0) * u + 0.2)
    return -u


ROOT = real_root()
LINEAR = 0.5 - ROOT
FREE = 0.2 - ROOT * LINEAR
REACH = 1.0 / LINEAR
SCALE = 2.0 * COULOMB / REACH**6
VMEM_LIMIT = 24 * 1024 * 1024
F32 = jnp.float32
BF16 = jnp.bfloat16


def fold(g, n):
    if n % 2:
        return g
    half = n // 2
    return (3 * half - 1 - g if g >= half else g) if isinstance(g, int) else jnp.where(g < half, g, 3 * half - 1 - g)


def tile_of(g, y, n):
    t = fold(g, n)
    if isinstance(y, int):
        return n - 1 - t if y % 2 else t
    return jnp.where(lax.rem(y, 2) == 1, n - 1 - t, t)


def device_of(t, y, n):
    if isinstance(y, int):
        return fold(n - 1 - t if y % 2 else t, n)
    return fold(jnp.where(lax.rem(y, 2) == 1, n - 1 - t, t), n)


def ring(n, k):
    return [(i, (i + k) % n) for i in range(n)]


def pieces_of(x):
    hi = x.astype(BF16)
    rest = x - hi.astype(F32)
    mid = rest.astype(BF16)
    low = (rest - mid.astype(F32)).astype(BF16)
    return hi, mid, low


def pick(species, table_ref):
    out = jnp.full(species.shape, table_ref[0], F32)
    for t in range(1, table_ref.shape[0]):
        out = jnp.where(species == t, table_ref[t], out)
    return out


def pack_kernel(pz, tz, off_ref, hist_ref, occ_ref, spec_ref, chi_ref, eta_ref, gam_ref, aux_ref, part_ref, *refs):
    tiles, cell_ref = refs[:-1], refs[-1]
    cells, slots = occ_ref.shape
    weight = occ_ref[...].astype(F32)
    species = spec_ref[...]
    predicted = WEIGHTS[0] * hist_ref[0]
    for level in range(1, len(WEIGHTS)):
        predicted = predicted + WEIGHTS[level] * hist_ref[level]
    predicted = weight * predicted
    chi = pick(species, chi_ref)
    eta = pick(species, eta_ref)
    gam = pick(species, gam_ref)
    root = lax.rsqrt(gam)
    shield = root * root * root * ((REACH / EDGE) ** 1.5)
    inverse = 1.0 / eta
    base = chi + eta * predicted - COULOMB * gam * predicted
    winv = weight * inverse
    zero = jnp.zeros((1, slots), F32)
    rows = [weight, weight * base, predicted, winv * base, winv]
    rows = [jnp.sum(r, axis=0, keepdims=True) for r in rows] + [zero] * 3
    part_ref[...] = jnp.broadcast_to(jnp.sum(jnp.concatenate(rows, axis=0), axis=1, keepdims=True), part_ref.shape)
    tri = lax.broadcasted_iota(jnp.int32, (slots, slots), 0) <= lax.broadcasted_iota(jnp.int32, (slots, slots), 1)
    wb = weight.astype(BF16)
    rank = jnp.dot(wb, tri.astype(F32).astype(BF16), preferred_element_type=F32)
    count = jnp.dot(wb, jnp.ones((slots, slots), BF16), preferred_element_type=F32)
    pos = jnp.where(weight > 0, rank - 1.0, -1.0)
    aux_ref[0] = base
    aux_ref[1] = predicted
    aux_ref[2] = inverse
    aux_ref[3] = pos
    fields = [off_ref[d] * (REACH / EDGE) for d in range(3)] + [predicted, shield, winv, weight, weight]
    row_id = lax.broadcasted_iota(jnp.int32, (slots, slots), 0).astype(F32)
    lane = lax.broadcasted_iota(jnp.int32, (FIELDS, slots), 1).astype(F32)
    sub = lax.broadcasted_iota(jnp.int32, (FIELDS, slots), 0)
    for c in range(cells):
        feat = jnp.concatenate([f[c : c + 1] for f in fields], axis=0)
        hot = jnp.where(row_id == pos[c : c + 1], 1.0, 0.0).astype(BF16)
        parts = jnp.concatenate(pieces_of(feat), axis=0)
        out = lax.dot_general(parts, hot, (((1,), (1,)), ((), ())), preferred_element_type=F32)
        out = out[:FIELDS] + out[FIELDS : 2 * FIELDS] + out[2 * FIELDS :]
        number = jnp.broadcast_to(count[c : c + 1], (FIELDS, slots))
        out = jnp.where((sub == 4) & (lane >= number), 1.0, out)
        cell_ref[c] = jnp.where(sub == 7, number, out)
    nx = len(tiles)
    me = lax.axis_index("gx")
    ty = tiles[0].shape[0]
    nz = tz * pz
    for k in range(nx):
        owner = tile_of(lax.rem(me + (nx - k), nx), lax.axis_index("gy"), nx)
        corner = (owner // pz) * (ty * nz) + (owner % pz) * tz
        for r in range(ty):
            for z in range(tz):
                tiles[k][r, z] = cell_ref[corner + (r * nz + z)]


def pair_kernel(cfg, *refs):
    nx, ty, tz, slots = cfg["nx"], cfg["ty"], cfg["tz"], cfg["slots"]
    shell, alone, group = cfg["shell"], cfg["alone"], cfg["group"]
    side, up, first = cfg["side"], cfg["up"], cfg["first"]
    refs = list(refs)
    planes = [refs.pop(0) for _ in range(nx)]
    edge_low, edge_high = (refs.pop(0), refs.pop(0)) if side else (None, None)
    above = refs.pop(0) if up else None
    before, part_ref = (None, None) if first else (refs.pop(0), refs.pop(0))
    out_ref, part_out = refs.pop(0), refs.pop(0)
    up_ref = refs.pop(0) if up else None
    abc, turned_ref, wide_ref, acca, accb, base_s, chunk_s, itemb_s, itemc_s = refs
    nck = slots // 8
    if up:
        me, y = lax.axis_index("gx"), lax.axis_index("gy")
        t = tile_of(me, y, nx) + cfg["pz"]
        y = lax.rem(y + jnp.where(t < nx, 0, 1), cfg["gy"])
        turn = device_of(lax.rem(t, nx), y, nx) - me
        there = [lax.rem(p - turn + 2 * nx, nx) for p in range(nx)]
    nb = nx * ty * len(cfg["mine"])
    z2 = tz + 2
    per = (ty + 1) * z2
    own = [(p, r, z) for p in range(nx) for r in range(ty) for z in cfg["mine"]]

    def cell_of(p, r, z):
        return (p % nx) * per + r * z2 + z + 1

    def load(p, r, z):
        if r < ty:
            return planes[p][r, z] if 0 <= z < tz else (edge_low[p, r] if z < 0 else edge_high[p, r])
        return above[there[p], z + 1]

    order = (0, 1, 2, 4, 3)
    total_chunks = jnp.int32(0)
    for b, (p, r, z) in enumerate(own):
        cell = load(p, r, z)
        turned_ref[b * nck : (b + 1) * nck] = cell.T.reshape(nck, 8, FIELDS)
        number = (jnp.max(cell[7:8]).astype(jnp.int32) + 7) // 8
        chunk_s[b] = number
        total_chunks = total_chunks + number
        for a in range(3):
            base_s[a * (nb + 1) + b] = cell_of(p + a - 1, r, z)
    chunk_s[nb] = 0
    for a in range(3):
        base_s[a * (nb + 1) + nb] = cell_of(0, 0, own[0][2])
    sub = lax.broadcasted_iota(jnp.int32, (8, slots), 0)
    slant = lax.broadcasted_iota(jnp.int32, (8, slots), 1) - sub
    blank = jnp.zeros((8, slots), F32)
    turned_ref[nb * nck] = jnp.where(lax.broadcasted_iota(jnp.int32, (8, FIELDS), 1) == 4, 1.0, 0.0)
    touched = {}
    for b, (p, r, z) in enumerate(own):
        for a, y, c in shell + ([(0, 0, 0)] if alone else []):
            touched[cell_of(p + a, r + y, z + c)] = ((p + a) % nx, r + y, z + c)
    for key, where in touched.items():
        cell = load(*where)
        for k, f in enumerate(order):
            abc[key, k] = jnp.broadcast_to(cell[f : f + 1], (8, slots))
    for b in range(nb + 1):
        for g in range(group):
            for q in range(len(shell)):
                acca[g, b, q] = blank

    def extend(t, b, c):
        for g in range(group):
            itemb_s[t * group + g] = b
            itemc_s[t * group + g] = c
            more = c + 1 < chunk_s[b]
            b, c = jnp.where(more, b, jnp.minimum(b + 1, nb)), jnp.where(more, c + 1, 0)
        return b, c

    def listed(t, g):
        return itemb_s[t * group + g], itemc_s[t * group + g]

    def prepare(t, g):
        b, c = listed(t, g)
        block = turned_ref[b * nck + c]
        for k, f in enumerate(order):
            wide_ref[g, k] = jnp.broadcast_to(block[:, f : f + 1], (8, slots))

    def value(ai, shift, bf):
        dx, dy, dz = [abc[ai, k] - bf[k][o] for k, o in enumerate(shift)]
        s = dx * dx + dy * dy + dz * dz
        s = jnp.minimum(jnp.maximum(s, 1e-12), REACH * REACH)
        u = s * lax.rsqrt(s)
        v = REACH - u
        v = v * v
        v = v * v
        x = s * u + abc[ai, 3] * bf[3]
        power = jnp.exp2(jnp.log2(x) * (-1.0 / 3.0))
        poly = (u + ROOT * REACH) * ((s + u) + FREE * REACH * REACH)
        return (v * poly) * power

    def based(t, g):
        b = listed(t, g)[0]
        return tuple(base_s[a * (nb + 1) + b] for a in range(3))

    def item(t, g, held):
        b, c = listed(t, g)
        bases = held if g == 0 else based(t, g)
        raw = [wide_ref[g, k] for k in range(5)]
        bf = [{o: (raw[k] - o * REACH if o else raw[k]) for o in (-1, 0, 1)} for k in range(3)] + [raw[3]]
        qb = raw[4]
        total = None
        if alone:
            total = value(bases[1], (0, 0, 0), bf) * abc[bases[1], 4]
        for q, (a, y, z) in enumerate(shell):
            ai = bases[a + 1] + (y * z2 + z)
            k = value(ai, (a, y, z), bf)
            term = k * abc[ai, 4]
            total = term if total is None else total + term
            acca[g, b, q] = acca[g, b, q] + k * qb
        accb[b * nck + c] = total

    def step(t, carry):
        for g in range(group):
            item(t, g, carry[2:])
        for g in range(group):
            prepare(t + 1, g)
        return extend(t + 2, *carry[:2]) + based(t + 1, 0)

    ahead = extend(1, *extend(0, jnp.int32(0), jnp.int32(0)))
    for g in range(group):
        prepare(0, g)
    steps = (total_chunks + (group - 1)) // group
    lax.fori_loop(0, steps, step, ahead + based(0, 0))

    sums = {}

    def add(key, term):
        sums[key] = sums[key] + term if key in sums else term

    for b, (p, r, z) in enumerate(own):
        rows = accb[b * nck : (b + 1) * nck].reshape(slots, slots).T
        folded = rows[:8]
        for i in range(1, nck):
            folded = folded + rows[8 * i : 8 * i + 8]
        filled = jnp.broadcast_to(load(p, r, z)[6:7], (8, slots)) > 0.0
        add(cell_of(p, r, z), jnp.where(filled, folded, 0.0))
        for g in range(group):
            for q, (a, y, c) in enumerate(shell):
                add(cell_of(p + a, r + y, z + c), acca[g, b, q])
    one = jnp.zeros((1, slots), F32)
    two = jnp.zeros((1, slots), F32)
    for p in range(nx):
        for r in range(ty + 1):
            for z in range(-1, tz + 1):
                key = cell_of(p, r, z)
                row = jnp.zeros((1, slots), F32)
                if key in sums:
                    row = jnp.sum(sums[key], axis=0, keepdims=True)
                    cell = load(p, r, z)
                    one = one + cell[6:7] * row
                    two = two + cell[5:6] * row
                i = r * z2 + z + 1
                if r == ty:
                    if up:
                        up_ref[there[p], z + 1 : z + 2, :] = row
                elif first:
                    out_ref[p, i : i + 1, :] = row
                else:
                    out_ref[p, i : i + 1, :] = before[p, i : i + 1, :] + row
    scale = SCALE
    none = jnp.zeros((1, slots), F32)
    rows = jnp.concatenate([none, scale * one, none, scale * two] + [none] * 4, axis=0)
    if not first:
        rows = rows + part_ref[...]
    if cfg["last"]:
        rows = jnp.broadcast_to(jnp.sum(rows, axis=1, keepdims=True), rows.shape)
    part_out[...] = rows


def pair_call(cfg, *args):
    nx, ty, tz, slots = cfg["nx"], cfg["ty"], cfg["tz"], cfg["slots"]
    nb = nx * ty * len(cfg["mine"])
    nck = slots // 8
    shape = lambda *s: jax.ShapeDtypeStruct(s, F32)
    vmem = pl.BlockSpec(memory_space=pltpu.VMEM)
    outs = [shape(nx, ty * (tz + 2), slots), shape(8, slots)]
    if cfg["up"]:
        outs.append(shape(nx, tz + 2, slots))
    return pl.pallas_call(
        lambda *refs: pair_kernel(cfg, *refs),
        out_shape=tuple(outs),
        in_specs=[vmem] * len(args),
        out_specs=(vmem,) * len(outs),
        scratch_shapes=[
            pltpu.VMEM((nx * (ty + 1) * (tz + 2), 5, 8, slots), F32),
            pltpu.VMEM((nb * nck + 1, 8, FIELDS), F32),
            pltpu.VMEM((cfg["group"], 5, 8, slots), F32),
            pltpu.VMEM((cfg["group"], nb + 1, len(cfg["shell"]), 8, slots), F32),
            pltpu.VMEM((nb * nck + 1, 8, slots), F32),
            pltpu.SMEM((3 * (nb + 1),), jnp.int32),
            pltpu.SMEM((nb + 1,), jnp.int32),
            pltpu.SMEM((nb * nck + 4 * cfg["group"],), jnp.int32),
            pltpu.SMEM((nb * nck + 4 * cfg["group"],), jnp.int32),
        ],
        compiler_params=pltpu.CompilerParams(vmem_limit_bytes=VMEM_LIMIT),
        name=cfg["name"],
    )(*args)


def unpack_kernel(sum_ref, aux_ref, out_ref):
    cells, slots = out_ref.shape
    row_id = lax.broadcasted_iota(jnp.int32, (slots, slots), 0).astype(F32)
    pos = aux_ref[3]
    hi, mid, low = [t.astype(F32) for t in pieces_of(sum_ref[...])]
    lines = []
    for c in range(cells):
        hot = jnp.where(row_id == pos[c : c + 1], 1.0, 0.0).astype(BF16)
        parts = jnp.concatenate([hi[c : c + 1], mid[c : c + 1], low[c : c + 1]] + [jnp.zeros((5, slots), F32)], axis=0)
        out = jnp.dot(parts.astype(BF16), hot, preferred_element_type=F32)
        lines.append(out[0:1] + out[1:2] + out[2:3])
    out_ref[...] = jnp.concatenate(lines, axis=0)


def body(offsets, history, occupied, species, chi_table, eta_table, gamma_table):
    _, ny, nz, slots = occupied.shape
    cells = ny * nz
    axes = ("gx", "gy", "gz")
    nx, gy, gz = [lax.axis_size(a) for a in axes]
    py = math.gcd(nx, ny)
    pz = nx // py
    ty, tz = ny // py, nz // pz
    z2 = tz + 2
    vmem = pl.BlockSpec(memory_space=pltpu.VMEM)
    shape = lambda *s: jax.ShapeDtypeStruct(s, F32)
    occ = occupied.reshape(cells, slots)
    aux, part, *tiles = pl.pallas_call(
        lambda *refs: pack_kernel(pz, tz, *refs),
        out_shape=(shape(4, cells, slots), shape(8, slots)) + (shape(ty, tz, FIELDS, slots),) * nx,
        in_specs=[vmem] * 4 + [pl.BlockSpec(memory_space=pltpu.SMEM)] * 3,
        out_specs=(vmem,) * (2 + nx),
        scratch_shapes=[pltpu.VMEM((cells, FIELDS, slots), F32)],
        name="pack",
    )(
        offsets.reshape(3, cells, slots),
        history.reshape(-1, cells, slots),
        occ,
        species.reshape(cells, slots),
        chi_table,
        eta_table,
        gamma_table,
    )
    me, column = lax.axis_index("gx"), lax.axis_index("gy")
    planes = [tiles[0]] + [lax.ppermute(tiles[k], "gx", ring(nx, -k)) for k in range(1, nx)]

    def number_of(x, y, z):
        return (x * gy + y) * gz + z

    def towards(up, side):
        pairs = []
        for x in range(nx):
            for y in range(gy):
                for z in range(gz):
                    t = tile_of(x, y, nx)
                    row = (y * py + t // pz + up) % (gy * py)
                    col = (z * pz + t % pz + side) % (gz * pz)
                    source = device_of(row % py * pz + col % pz, row // py, nx)
                    pairs.append((number_of(source, row // py, col // pz), number_of(x, y, z)))
        return pairs

    def turned(array, side):
        if pz == 1:
            return array
        t = tile_of(me, column, nx)
        t = t - t % pz + (t + side) % pz
        return jnp.roll(array, device_of(t, column, nx) - me, axis=0)

    first = jnp.stack([p[:, 0] for p in planes])
    last = jnp.stack([p[:, tz - 1] for p in planes])
    if gz * pz == 2:
        both = lax.ppermute(jnp.stack([first, last]), axes, towards(0, 1))
        edge_low, edge_high = turned(both[1], -1), turned(both[0], 1)
    else:
        edge_low = turned(lax.ppermute(last, axes, towards(0, -1)), -1)
        edge_high = turned(lax.ppermute(first, axes, towards(0, 1)), 1)
    bottom = jnp.concatenate([edge_low[:, :1], jnp.stack([p[0] for p in planes]), edge_high[:, :1]], axis=1)
    above = lax.ppermute(bottom, axes, towards(1, 0))

    common = dict(nx=nx, ty=ty, tz=tz, slots=slots, pz=pz, gy=gy)
    half = tz // 2
    row = dict(common, shell=SHELL_ROW, alone=True, group=ROW_GROUP, side=True, up=False)
    early = dict(row, name="early", mine=range(half), first=True, last=False)
    late = dict(row, name="late", mine=range(half, tz), first=False, last=True)
    upper = dict(common, name="upper", mine=range(tz), shell=SHELL_UP, alone=False, group=UP_GROUP, side=ty > 1, up=True, first=False, last=False)
    sums, found = pair_call(early, *planes, edge_low, edge_high)
    inner_edges = (edge_low, edge_high) if ty > 1 else ()
    sums, found, up_sums = pair_call(upper, *planes, *inner_edges, above, sums, found)
    back = lax.ppermute(up_sums, axes, [(t, s) for s, t in towards(1, 0)])
    sums, found = pair_call(late, *planes, edge_low, edge_high, sums, found)
    part = part + found

    sums = jnp.concatenate([sums[:, :z2] + back, sums[:, z2:], jnp.broadcast_to(part, (nx,) + part.shape)], axis=1)
    rows = ty * z2
    gathered = [sums[0]] + [lax.ppermute(sums[k], "gx", ring(nx, k)) for k in range(1, nx)]
    total = gathered[0][rows:]
    for g in gathered[1:]:
        total = total + g[rows:]
    for axis, count in (("gz", gz), ("gy", gy)):
        if count & (count - 1):
            total = lax.psum(total, axis)
        else:
            for bit in range(count.bit_length() - 1):
                total = total + lax.ppermute(total, axis, [(i, i ^ (1 << bit)) for i in range(count)])
    wide = jnp.zeros((ny, nz + 2, slots), F32)
    for k in range(nx):
        owner = tile_of((me - k) % nx, column, nx)
        at = ((owner // pz) * ty, (owner % pz) * tz, 0)
        piece = gathered[k][:rows].reshape(ty, z2, slots)
        wide = wide + lax.dynamic_update_slice(jnp.zeros_like(wide), piece, at)
    if gz == 2:
        both = lax.ppermute(jnp.stack([wide[:, 0], wide[:, nz + 1]]), "gz", ring(gz, 1))
        from_high, from_low = both[0], both[1]
    else:
        from_high = lax.ppermute(wide[:, 0], "gz", ring(gz, -1))
        from_low = lax.ppermute(wide[:, nz + 1], "gz", ring(gz, 1))
    inner = wide[:, 1 : nz + 1]
    inner = jnp.concatenate(
        [inner[:, :1] + from_low[:, None], inner[:, 1 : nz - 1], inner[:, nz - 1 :] + from_high[:, None]], axis=1
    )
    summed = pl.pallas_call(
        unpack_kernel,
        out_shape=shape(cells, slots),
        in_specs=[vmem] * 2,
        out_specs=vmem,
        compiler_params=pltpu.CompilerParams(vmem_limit_bytes=VMEM_LIMIT),
        name="unpack",
    )(inner.reshape(cells, slots), aux)
    weight = occ.astype(F32)
    number, elec, charge_sum, scaled, inv_sum = [total[i : i + 1] for i in range(5)]
    chem = elec / number
    stepped_total = charge_sum - scaled + chem * inv_sum
    delta = aux[0] + SCALE * summed - chem
    stepped = weight * (aux[1] - delta * aux[2])
    charge = weight * (stepped - stepped_total / number)
    residual = weight * delta
    return charge.reshape(occupied.shape), residual.reshape(occupied.shape)


def solution(mesh):
    return jax.shard_map(
        body,
        mesh=mesh,
        in_specs=(
            P(None, "gx", "gy", "gz", None),
            P(None, "gx", "gy", "gz", None),
            P("gx", "gy", "gz", None),
            P("gx", "gy", "gz", None),
            P(),
            P(),
            P(),
        ),
        out_specs=(P("gx", "gy", "gz", None), P("gx", "gy", "gz", None)),
        check_vma=False,
    )
```

```python
import math

import jax
import jax.numpy as jnp
from jax import lax
from jax.experimental import pallas as pl
from jax.experimental.pallas import tpu as pltpu
from jax.sharding import PartitionSpec as P

EDGE = 10.0
COULOMB = 14.4
WEIGHTS = (22.0 / 7.0, -55.0 / 14.0, 55.0 / 21.0, -22.0 / 21.0, 5.0 / 21.0, -1.0 / 42.0)
FIELDS = 8
SHELL_UP = [(a, 1, c) for a in (-1, 0, 1) for c in (-1, 0, 1)]
SHELL_ROW = [(a, 0, 1) for a in (-1, 0, 1)] + [(1, 0, 0)]
UP_GROUP, ROW_GROUP = 3, 8


def real_root():
    u = -0.34
    for _ in range(8):
        u -= (((u + 0.5) * u + 0.2) * u + 0.05) / ((3.0 * u + 1.0) * u + 0.2)
    return -u


ROOT = real_root()
LINEAR = 0.5 - ROOT
FREE = 0.2 - ROOT * LINEAR
REACH = 1.0 / LINEAR
SCALE = 2.0 * COULOMB / REACH**6
VMEM_LIMIT = 24 * 1024 * 1024
F32 = jnp.float32
BF16 = jnp.bfloat16


def fold(g, n):
    if n % 2:
        return g
    half = n // 2
    return (3 * half - 1 - g if g >= half else g) if isinstance(g, int) else jnp.where(g < half, g, 3 * half - 1 - g)


def tile_of(g, y, n):
    t = fold(g, n)
    if isinstance(y, int):
        return n - 1 - t if y % 2 else t
    return jnp.where(lax.rem(y, 2) == 1, n - 1 - t, t)


def device_of(t, y, n):
    if isinstance(y, int):
        return fold(n - 1 - t if y % 2 else t, n)
    return fold(jnp.where(lax.rem(y, 2) == 1, n - 1 - t, t), n)


def ring(n, k):
    return [(i, (i + k) % n) for i in range(n)]


def pieces_of(x):
    hi = x.astype(BF16)
    rest = x - hi.astype(F32)
    mid = rest.astype(BF16)
    low = (rest - mid.astype(F32)).astype(BF16)
    return hi, mid, low


def pick(species, table_ref):
    out = jnp.full(species.shape, table_ref[0], F32)
    for t in range(1, table_ref.shape[0]):
        out = jnp.where(species == t, table_ref[t], out)
    return out


def pack_kernel(pz, tz, off_ref, hist_ref, occ_ref, spec_ref, chi_ref, eta_ref, gam_ref, aux_ref, part_ref, *refs):
    tiles, cell_ref = refs[:-1], refs[-1]
    cells, slots = occ_ref.shape
    weight = occ_ref[...].astype(F32)
    species = spec_ref[...]
    predicted = WEIGHTS[0] * hist_ref[0]
    for level in range(1, len(WEIGHTS)):
        predicted = predicted + WEIGHTS[level] * hist_ref[level]
    predicted = weight * predicted
    chi = pick(species, chi_ref)
    eta = pick(species, eta_ref)
    gam = pick(species, gam_ref)
    root = lax.rsqrt(gam)
    shield = root * root * root * ((REACH / EDGE) ** 1.5)
    inverse = 1.0 / eta
    base = chi + eta * predicted - COULOMB * gam * predicted
    winv = weight * inverse
    zero = jnp.zeros((1, slots), F32)
    rows = [weight, weight * base, predicted, winv * base, winv]
    rows = [jnp.sum(r, axis=0, keepdims=True) for r in rows] + [zero] * 3
    part_ref[...] = jnp.broadcast_to(jnp.sum(jnp.concatenate(rows, axis=0), axis=1, keepdims=True), part_ref.shape)
    tri = lax.broadcasted_iota(jnp.int32, (slots, slots), 0) <= lax.broadcasted_iota(jnp.int32, (slots, slots), 1)
    wb = weight.astype(BF16)
    rank = jnp.dot(wb, tri.astype(F32).astype(BF16), preferred_element_type=F32)
    count = jnp.dot(wb, jnp.ones((slots, slots), BF16), preferred_element_type=F32)
    pos = jnp.where(weight > 0, rank - 1.0, -1.0)
    aux_ref[0] = base
    aux_ref[1] = predicted
    aux_ref[2] = inverse
    aux_ref[3] = pos
    fields = [off_ref[d] * (REACH / EDGE) for d in range(3)] + [predicted, shield, winv, weight, weight]
    row_id = lax.broadcasted_iota(jnp.int32, (slots, slots), 0).astype(F32)
    lane = lax.broadcasted_iota(jnp.int32, (FIELDS, slots), 1).astype(F32)
    sub = lax.broadcasted_iota(jnp.int32, (FIELDS, slots), 0)
    for c in range(cells):
        feat = jnp.concatenate([f[c : c + 1] for f in fields], axis=0)
        hot = jnp.where(row_id == pos[c : c + 1], 1.0, 0.0).astype(BF16)
        parts = jnp.concatenate(pieces_of(feat), axis=0)
        out = lax.dot_general(parts, hot, (((1,), (1,)), ((), ())), preferred_element_type=F32)
        out = out[:FIELDS] + out[FIELDS : 2 * FIELDS] + out[2 * FIELDS :]
        number = jnp.broadcast_to(count[c : c + 1], (FIELDS, slots))
        out = jnp.where((sub == 4) & (lane >= number), 1.0, out)
        cell_ref[c] = jnp.where(sub == 7, number, out)
    nx = len(tiles)
    me = lax.axis_index("gx")
    ty = tiles[0].shape[0]
    nz = tz * pz
    for k in range(nx):
        owner = tile_of(lax.rem(me + (nx - k), nx), lax.axis_index("gy"), nx)
        corner = (owner // pz) * (ty * nz) + (owner % pz) * tz
        for r in range(ty):
            for z in range(tz):
                tiles[k][r, z] = cell_ref[corner + (r * nz + z)]


def pair_kernel(cfg, *refs):
    nx, ty, tz, slots = cfg["nx"], cfg["ty"], cfg["tz"], cfg["slots"]
    shell, alone, group = cfg["shell"], cfg["alone"], cfg["group"]
    side, up, first = cfg["side"], cfg["up"], cfg["first"]
    refs = list(refs)
    planes = [refs.pop(0) for _ in range(nx)]
    edge_low, edge_high = (refs.pop(0), refs.pop(0)) if side else (None, None)
    above = refs.pop(0) if up else None
    before, part_ref = (None, None) if first else (refs.pop(0), refs.pop(0))
    out_ref, part_out = refs.pop(0), refs.pop(0)
    up_ref = refs.pop(0) if up else None
    abc, turned_ref, wide_ref, acca, accb, base_s, chunk_s, itemb_s, itemc_s = refs
    nck = slots // 8
    if up:
        me, y = lax.axis_index("gx"), lax.axis_index("gy")
        t = tile_of(me, y, nx) + cfg["pz"]
        y = lax.rem(y + jnp.where(t < nx, 0, 1), cfg["gy"])
        turn = device_of(lax.rem(t, nx), y, nx) - me
        there = [lax.rem(p - turn + 2 * nx, nx) for p in range(nx)]
    nb = nx * ty * len(cfg["mine"])
    z2 = tz + 2
    per = (ty + 1) * z2
    own = [(p, r, z) for p in range(nx) for r in range(ty) for z in cfg["mine"]]

    def cell_of(p, r, z):
        return (p % nx) * per + r * z2 + z + 1

    def load(p, r, z):
        if r < ty:
            return planes[p][r, z] if 0 <= z < tz else (edge_low[p, r] if z < 0 else edge_high[p, r])
        return above[there[p], z + 1]

    order = (0, 1, 2, 4, 3)
    total_chunks = jnp.int32(0)
    for b, (p, r, z) in enumerate(own):
        cell = load(p, r, z)
        turned_ref[b * nck : (b + 1) * nck] = cell.T.reshape(nck, 8, FIELDS)
        number = (jnp.max(cell[7:8]).astype(jnp.int32) + 7) // 8
        chunk_s[b] = number
        total_chunks = total_chunks + number
        for a in range(3):
            base_s[a * (nb + 1) + b] = cell_of(p + a - 1, r, z)
    chunk_s[nb] = 0
    for a in range(3):
        base_s[a * (nb + 1) + nb] = cell_of(0, 0, own[0][2])
    sub = lax.broadcasted_iota(jnp.int32, (8, slots), 0)
    slant = lax.broadcasted_iota(jnp.int32, (8, slots), 1) - sub
    blank = jnp.zeros((8, slots), F32)
    turned_ref[nb * nck] = jnp.where(lax.broadcasted_iota(jnp.int32, (8, FIELDS), 1) == 4, 1.0, 0.0)
    touched = {}
    for b, (p, r, z) in enumerate(own):
        for a, y, c in shell + ([(0, 0, 0)] if alone else []):
            touched[cell_of(p + a, r + y, z + c)] = ((p + a) % nx, r + y, z + c)
    for key, where in touched.items():
        cell = load(*where)
        for k, f in enumerate(order):
            abc[key, k] = jnp.broadcast_to(cell[f : f + 1], (8, slots))
    for b in range(nb + 1):
        for g in range(group):
            for q in range(len(shell)):
                acca[g, b, q] = blank

    def extend(t, b, c):
        for g in range(group):
            itemb_s[t * group + g] = b
            itemc_s[t * group + g] = c
            more = c + 1 < chunk_s[b]
            b, c = jnp.where(more, b, jnp.minimum(b + 1, nb)), jnp.where(more, c + 1, 0)
        return b, c

    def listed(t, g):
        return itemb_s[t * group + g], itemc_s[t * group + g]

    def prepare(t, g):
        b, c = listed(t, g)
        block = turned_ref[b * nck + c]
        for k, f in enumerate(order):
            wide_ref[g, k] = jnp.broadcast_to(block[:, f : f + 1], (8, slots))

    def value(ai, shift, bf):
        dx, dy, dz = [abc[ai, k] - bf[k][o] for k, o in enumerate(shift)]
        s = dx * dx + dy * dy + dz * dz
        s = jnp.minimum(jnp.maximum(s, 1e-12), REACH * REACH)
        u = s * lax.rsqrt(s)
        v = REACH - u
        v = v * v
        v = v * v
        x = s * u + abc[ai, 3] * bf[3]
        power = jnp.exp2(jnp.log2(x) * (-1.0 / 3.0))
        poly = (u + ROOT * REACH) * ((s + u) + FREE * REACH * REACH)
        return (v * poly) * power

    def based(t, g):
        b = listed(t, g)[0]
        return tuple(base_s[a * (nb + 1) + b] for a in range(3))

    def item(t, g, held):
        b, c = listed(t, g)
        bases = held if g == 0 else based(t, g)
        raw = [wide_ref[g, k] for k in range(5)]
        bf = [{o: (raw[k] - o * REACH if o else raw[k]) for o in (-1, 0, 1)} for k in range(3)] + [raw[3]]
        qb = raw[4]
        total = None
        if alone:
            total = value(bases[1], (0, 0, 0), bf) * abc[bases[1], 4]
        for q, (a, y, z) in enumerate(shell):
            ai = bases[a + 1] + (y * z2 + z)
            k = value(ai, (a, y, z), bf)
            term = k * abc[ai, 4]
            total = term if total is None else total + term
            acca[g, b, q] = acca[g, b, q] + k * qb
        accb[b * nck + c] = total

    def step(t, carry):
        for g in range(group):
            item(t, g, carry[2:])
        for g in range(group):
            prepare(t + 1, g)
        return extend(t + 2, *carry[:2]) + based(t + 1, 0)

    ahead = extend(1, *extend(0, jnp.int32(0), jnp.int32(0)))
    for g in range(group):
        prepare(0, g)
    steps = (total_chunks + (group - 1)) // group
    lax.fori_loop(0, steps, step, ahead + based(0, 0))

    sums = {}

    def add(key, term):
        sums[key] = sums[key] + term if key in sums else term

    for b, (p, r, z) in enumerate(own):
        rows = accb[b * nck : (b + 1) * nck].reshape(slots, slots).T
        folded = rows[:8]
        for i in range(1, nck):
            folded = folded + rows[8 * i : 8 * i + 8]
        filled = jnp.broadcast_to(load(p, r, z)[6:7], (8, slots)) > 0.0
        add(cell_of(p, r, z), jnp.where(filled, folded, 0.0))
        for g in range(group):
            for q, (a, y, c) in enumerate(shell):
                add(cell_of(p + a, r + y, z + c), acca[g, b, q])
    one = jnp.zeros((1, slots), F32)
    two = jnp.zeros((1, slots), F32)
    for p in range(nx):
        for r in range(ty + 1):
            for z in range(-1, tz + 1):
                key = cell_of(p, r, z)
                row = jnp.zeros((1, slots), F32)
                if key in sums:
                    row = jnp.sum(sums[key], axis=0, keepdims=True)
                    cell = load(p, r, z)
                    one = one + cell[6:7] * row
                    two = two + cell[5:6] * row
                i = r * z2 + z + 1
                if r == ty:
                    if up:
                        up_ref[there[p], z + 1 : z + 2, :] = row
                elif first:
                    out_ref[p, i : i + 1, :] = row
                else:
                    out_ref[p, i : i + 1, :] = before[p, i : i + 1, :] + row
    scale = SCALE
    none = jnp.zeros((1, slots), F32)
    rows = jnp.concatenate([none, scale * one, none, scale * two] + [none] * 4, axis=0)
    if not first:
        rows = rows + part_ref[...]
    if cfg["last"]:
        rows = jnp.broadcast_to(jnp.sum(rows, axis=1, keepdims=True), rows.shape)
    part_out[...] = rows


def pair_call(cfg, *args):
    nx, ty, tz, slots = cfg["nx"], cfg["ty"], cfg["tz"], cfg["slots"]
    nb = nx * ty * len(cfg["mine"])
    nck = slots // 8
    shape = lambda *s: jax.ShapeDtypeStruct(s, F32)
    vmem = pl.BlockSpec(memory_space=pltpu.VMEM)
    outs = [shape(nx, ty * (tz + 2), slots), shape(8, slots)]
    if cfg["up"]:
        outs.append(shape(nx, tz + 2, slots))
    return pl.pallas_call(
        lambda *refs: pair_kernel(cfg, *refs),
        out_shape=tuple(outs),
        in_specs=[vmem] * len(args),
        out_specs=(vmem,) * len(outs),
        scratch_shapes=[
            pltpu.VMEM((nx * (ty + 1) * (tz + 2), 5, 8, slots), F32),
            pltpu.VMEM((nb * nck + 1, 8, FIELDS), F32),
            pltpu.VMEM((cfg["group"], 5, 8, slots), F32),
            pltpu.VMEM((cfg["group"], nb + 1, len(cfg["shell"]), 8, slots), F32),
            pltpu.VMEM((nb * nck + 1, 8, slots), F32),
            pltpu.SMEM((3 * (nb + 1),), jnp.int32),
            pltpu.SMEM((nb + 1,), jnp.int32),
            pltpu.SMEM((nb * nck + 4 * cfg["group"],), jnp.int32),
            pltpu.SMEM((nb * nck + 4 * cfg["group"],), jnp.int32),
        ],
        compiler_params=pltpu.CompilerParams(vmem_limit_bytes=VMEM_LIMIT),
        name=cfg["name"],
    )(*args)


def unpack_kernel(sum_ref, aux_ref, out_ref):
    cells, slots = out_ref.shape
    row_id = lax.broadcasted_iota(jnp.int32, (slots, slots), 0).astype(F32)
    pos = aux_ref[3]
    hi, mid, low = [t.astype(F32) for t in pieces_of(sum_ref[...])]
    lines = []
    for c in range(cells):
        hot = jnp.where(row_id == pos[c : c + 1], 1.0, 0.0).astype(BF16)
        parts = jnp.concatenate([hi[c : c + 1], mid[c : c + 1], low[c : c + 1]] + [jnp.zeros((5, slots), F32)], axis=0)
        out = jnp.dot(parts.astype(BF16), hot, preferred_element_type=F32)
        lines.append(out[0:1] + out[1:2] + out[2:3])
    out_ref[...] = jnp.concatenate(lines, axis=0)


def body(offsets, history, occupied, species, chi_table, eta_table, gamma_table):
    _, ny, nz, slots = occupied.shape
    cells = ny * nz
    axes = ("gx", "gy", "gz")
    nx, gy, gz = [lax.axis_size(a) for a in axes]
    py = math.gcd(nx, ny)
    pz = nx // py
    ty, tz = ny // py, nz // pz
    z2 = tz + 2
    vmem = pl.BlockSpec(memory_space=pltpu.VMEM)
    shape = lambda *s: jax.ShapeDtypeStruct(s, F32)
    occ = occupied.reshape(cells, slots)
    aux, part, *tiles = pl.pallas_call(
        lambda *refs: pack_kernel(pz, tz, *refs),
        out_shape=(shape(4, cells, slots), shape(8, slots)) + (shape(ty, tz, FIELDS, slots),) * nx,
        in_specs=[vmem] * 4 + [pl.BlockSpec(memory_space=pltpu.SMEM)] * 3,
        out_specs=(vmem,) * (2 + nx),
        scratch_shapes=[pltpu.VMEM((cells, FIELDS, slots), F32)],
        name="pack",
    )(
        offsets.reshape(3, cells, slots),
        history.reshape(-1, cells, slots),
        occ,
        species.reshape(cells, slots),
        chi_table,
        eta_table,
        gamma_table,
    )
    me, column = lax.axis_index("gx"), lax.axis_index("gy")
    planes = [tiles[0]] + [lax.ppermute(tiles[k], "gx", ring(nx, -k)) for k in range(1, nx)]

    def number_of(x, y, z):
        return (x * gy + y) * gz + z

    def towards(up, side):
        pairs = []
        for x in range(nx):
            for y in range(gy):
                for z in range(gz):
                    t = tile_of(x, y, nx)
                    row = (y * py + t // pz + up) % (gy * py)
                    col = (z * pz + t % pz + side) % (gz * pz)
                    source = device_of(row % py * pz + col % pz, row // py, nx)
                    pairs.append((number_of(source, row // py, col // pz), number_of(x, y, z)))
        return pairs

    def turned(array, side):
        if pz == 1:
            return array
        t = tile_of(me, column, nx)
        t = t - t % pz + (t + side) % pz
        return jnp.roll(array, device_of(t, column, nx) - me, axis=0)

    first = jnp.stack([p[:, 0] for p in planes])
    last = jnp.stack([p[:, tz - 1] for p in planes])
    if gz * pz == 2:
        both = lax.ppermute(jnp.stack([first, last]), axes, towards(0, 1))
        edge_low, edge_high = turned(both[1], -1), turned(both[0], 1)
    else:
        edge_low = turned(lax.ppermute(last, axes, towards(0, -1)), -1)
        edge_high = turned(lax.ppermute(first, axes, towards(0, 1)), 1)
    bottom = jnp.concatenate([edge_low[:, :1], jnp.stack([p[0] for p in planes]), edge_high[:, :1]], axis=1)
    above = lax.ppermute(bottom, axes, towards(1, 0))

    common = dict(nx=nx, ty=ty, tz=tz, slots=slots, pz=pz, gy=gy)
    half = tz // 2
    row = dict(common, shell=SHELL_ROW, alone=True, group=ROW_GROUP, side=True, up=False)
    early = dict(row, name="early", mine=range(half), first=True, last=False)
    late = dict(row, name="late", mine=range(half, tz), first=False, last=True)
    upper = dict(common, name="upper", mine=range(tz), shell=SHELL_UP, alone=False, group=UP_GROUP, side=ty > 1, up=True, first=False, last=False)
    sums, found = pair_call(early, *planes, edge_low, edge_high)
    inner_edges = (edge_low, edge_high) if ty > 1 else ()
    sums, found, up_sums = pair_call(upper, *planes, *inner_edges, above, sums, found)
    back = lax.ppermute(up_sums, axes, [(t, s) for s, t in towards(1, 0)])
    sums, found = pair_call(late, *planes, edge_low, edge_high, sums, found)
    part = part + found

    sums = jnp.concatenate([sums[:, :z2] + back, sums[:, z2:], jnp.broadcast_to(part, (nx,) + part.shape)], axis=1)
    rows = ty * z2
    gathered = [sums[0]] + [lax.ppermute(sums[k], "gx", ring(nx, k)) for k in range(1, nx)]
    total = gathered[0][rows:]
    for g in gathered[1:]:
        total = total + g[rows:]
    bits = [("gz", 1 << i) for i in range((gz - 1).bit_length())] + [("gy", 1 << i) for i in range((gy - 1).bit_length())]
    if gz & (gz - 1) or gy & (gy - 1):
        total = lax.psum(total, ("gy", "gz"))
        bits = []
    while bits:
        chosen, bits = bits[:2], bits[2:]
        masks = [bit * (gz if axis == "gy" else 1) for axis, bit in chosen]
        masks = masks + ([masks[0] | masks[1]] if len(masks) == 2 else [])
        moved = [lax.ppermute(total, ("gy", "gz"), [(i, i ^ m) for i in range(gy * gz)]) for m in masks]
        for other in moved:
            total = total + other
    wide = jnp.zeros((ny, nz + 2, slots), F32)
    for k in range(nx):
        owner = tile_of((me - k) % nx, column, nx)
        at = ((owner // pz) * ty, (owner % pz) * tz, 0)
        piece = gathered[k][:rows].reshape(ty, z2, slots)
        wide = wide + lax.dynamic_update_slice(jnp.zeros_like(wide), piece, at)
    if gz == 2:
        both = lax.ppermute(jnp.stack([wide[:, 0], wide[:, nz + 1]]), "gz", ring(gz, 1))
        from_high, from_low = both[0], both[1]
    else:
        from_high = lax.ppermute(wide[:, 0], "gz", ring(gz, -1))
        from_low = lax.ppermute(wide[:, nz + 1], "gz", ring(gz, 1))
    inner = wide[:, 1 : nz + 1]
    inner = jnp.concatenate(
        [inner[:, :1] + from_low[:, None], inner[:, 1 : nz - 1], inner[:, nz - 1 :] + from_high[:, None]], axis=1
    )
    summed = pl.pallas_call(
        unpack_kernel,
        out_shape=shape(cells, slots),
        in_specs=[vmem] * 2,
        out_specs=vmem,
        compiler_params=pltpu.CompilerParams(vmem_limit_bytes=VMEM_LIMIT),
        name="unpack",
    )(inner.reshape(cells, slots), aux)
    weight = occ.astype(F32)
    number, elec, charge_sum, scaled, inv_sum = [total[i : i + 1] for i in range(5)]
    chem = elec / number
    stepped_total = charge_sum - scaled + chem * inv_sum
    delta = aux[0] + SCALE * summed - chem
    stepped = weight * (aux[1] - delta * aux[2])
    charge = weight * (stepped - stepped_total / number)
    residual = weight * delta
    return charge.reshape(occupied.shape), residual.reshape(occupied.shape)


def solution(mesh):
    return jax.shard_map(
        body,
        mesh=mesh,
        in_specs=(
            P(None, "gx", "gy", "gz", None),
            P(None, "gx", "gy", "gz", None),
            P("gx", "gy", "gz", None),
            P("gx", "gy", "gz", None),
            P(),
            P(),
            P(),
        ),
        out_specs=(P("gx", "gy", "gz", None), P("gx", "gy", "gz", None)),
        check_vma=False,
    )
```
